256 devices in a mesh: col: 64 (over z, y, core), row: 4 (over x).
Axes of the slice: x: 4, y: 4, z: 8, core: 2. Of those that a mesh axis runs over, the one named last changes fastest.
Arguments:
- produced_encoder_vectors: bfloat16 [8192, 2048], P(('col', 'row')), may hold values from -7 to 7
- real_embeddings: bfloat16 [8192, 2048], P(('col', 'row')), may hold values from -7 to 7
Outputs:
- drift: float32 [8192, 2048], P(('col', 'row'))
The draws below stay inside these ranges and needn't reach their ends.
All inputs are finite; a program needn't handle non-finite values.
Results may differ from the reference program's by a relative error of at most 0.0035.
Values may be sent and summed in bfloat16 or wider, within the bound.
A program may use at most 64 MiB of HBM per device.

```python
import math
import jax
import jax.numpy as jnp
from jax import lax

D = 2048
NG = 8192
NR = 8192


def feature_pair(key):
    base_key = jax.random.fold_in(key, 11)
    random_seed_sequence = jax.random.split(base_key, 3)
    generated = jnp.clip(jax.random.normal(random_seed_sequence[0], (NG, D), jnp.float32), -6.0, 6.0)
    real_rows = jnp.clip(jax.random.normal(random_seed_sequence[2], (NR, D), jnp.float32), -6.0, 6.0)
    return (jnp.clip(generated, -7.0, 7.0), jnp.clip(real_rows, -7.0, 7.0))


def draw_produced_encoder_vectors(key, part):
    return feature_pair(key)[0].astype(jnp.bfloat16)


def draw_real_embeddings(key, part):
    return feature_pair(key)[1].astype(jnp.bfloat16)


def setup_inputs(seed: int = 0) -> dict:
    keys = jax.random.split(jax.random.key(seed), 3)
    return {
        "produced_encoder_vectors": draw_produced_encoder_vectors(jax.random.fold_in(keys[2], 71), 0),
        "real_embeddings": draw_real_embeddings(jax.random.fold_in(keys[2], 71), 0),
    }


laplace_scale_factor = 0.3
masked_logit = -1e+30
epsilon = 1e-06

def reference(produced_encoder_vectors, real_embeddings):
    samples = jnp.concatenate([produced_encoder_vectors, real_embeddings], axis=0)
    sample_sq = lax.optimization_barrier(jnp.sum(jnp.square(samples.astype(jnp.float32)), axis=1))
    gen_sq = lax.optimization_barrier(jnp.sum(jnp.square(produced_encoder_vectors.astype(jnp.float32)), axis=1))
    col_ids = jnp.concatenate([jnp.arange(NG, dtype=jnp.int32), jnp.full((NR,), -1, jnp.int32)])
    real_column = jnp.arange(NG + NR, dtype=jnp.int32) >= NG
    block_rows = math.gcd(NG, 512)
    block_count = NG // block_rows

    def logits_of(first_row):
        row_feats = lax.dynamic_slice_in_dim(produced_encoder_vectors, first_row, block_rows, 0)
        row_sq = lax.dynamic_slice_in_dim(gen_sq, first_row, block_rows, 0)
        row_ids = first_row + jnp.arange(block_rows, dtype=jnp.int32)
        inner_prod = jnp.dot(row_feats, samples.T, preferred_element_type=jnp.float32)
        pairwise_gap_norms = row_sq[:, None] + sample_sq[None, :] - 2.0 * inner_prod
        similarity_weights = -jnp.sqrt(jnp.maximum(pairwise_gap_norms, 1.0)) / laplace_scale_factor
        return jnp.where(row_ids[:, None] == col_ids[None, :], masked_logit, similarity_weights)

    def column_step(running, block_index):
        target_maximum_logit, col_total = running
        similarity_weights = logits_of((block_index * block_rows).astype(jnp.int32))
        block_peak = lax.optimization_barrier(jnp.max(similarity_weights, axis=0))
        block_total = lax.optimization_barrier(jnp.sum(jnp.exp(similarity_weights - block_peak[None, :]), axis=0))
        updated_highest_logit = jnp.maximum(target_maximum_logit, block_peak)
        new_total = col_total * jnp.exp(target_maximum_logit - updated_highest_logit) + block_total * jnp.exp(block_peak - updated_highest_logit)
        return ((updated_highest_logit, new_total), None)
    start = (jnp.full((NG + NR,), masked_logit, jnp.float32), jnp.zeros((NG + NR,), jnp.float32))
    (target_maximum_logit, col_total), _ = lax.scan(column_step, start, jnp.arange(block_count, dtype=jnp.int32))
    col_shift = target_maximum_logit + jnp.log(col_total)

    def drift_of(block_index):
        similarity_weights = logits_of((block_index * block_rows).astype(jnp.int32))
        row_peak = lax.optimization_barrier(jnp.max(similarity_weights, axis=1))
        row_sum = lax.optimization_barrier(jnp.sum(jnp.exp(similarity_weights - row_peak[:, None]), axis=1))
        half = jnp.exp(similarity_weights - 0.5 * row_peak[:, None] - 0.5 * col_shift[None, :])
        gen_mass = lax.optimization_barrier(jnp.sum(jnp.where(real_column[None, :], 0.0, half), axis=1))
        real_mass = lax.optimization_barrier(jnp.sum(jnp.where(real_column[None, :], half, 0.0), axis=1))
        signed_scale = jnp.where(real_column[None, :], gen_mass[:, None], -real_mass[:, None]) / row_sum[:, None]
        signed = (half * signed_scale).astype(jnp.bfloat16)
        return jnp.dot(signed, samples, preferred_element_type=jnp.float32)
    raw = lax.map(drift_of, jnp.arange(block_count, dtype=jnp.int32)).reshape(NG, D)
    drift_potential = jnp.sum(raw * raw)
    return raw / jnp.sqrt(drift_potential / (NG * D) + epsilon)
```

```python
import functools

import jax
import jax.numpy as jnp
from jax import lax
from jax.experimental import pallas as pl
from jax.experimental.pallas import tpu as pltpu
from jax.sharding import Mesh
from jax.sharding import PartitionSpec as P

AXES = ("z", "y", "c", "x")
NZ, NY, NC, NX = 8, 4, 2, 4
PER = 32
WIDTH = 2048
ROWS = NX * NY * PER
CHUNK = 2 * NC * PER
COLS = NZ * CHUNK
INV_SCALE = 1.0 / 0.3
MASKED = -1e30
EPS = 1e-6
F32 = jnp.float32
BF16 = jnp.bfloat16


def eye():
    return lax.broadcasted_iota(jnp.int32, (128, 128), 0) == lax.broadcasted_iota(
        jnp.int32, (128, 128), 1
    )


def to_lanes(v):
    return jnp.sum(jnp.where(eye(), jnp.broadcast_to(v, (128, 128)), 0.0), axis=0, keepdims=True)


def to_rows(v):
    return jnp.sum(jnp.where(eye(), jnp.broadcast_to(v, (128, 128)), 0.0), axis=1, keepdims=True)


def kernel(
    gen_ref, real_ref, out_ref,
    rows, cols, logits, signed, rsq, rvec, gvec, mvec, csv,
    cstat, rstat, mstat, n1, n2,
    psend, acc, far1, near1, qsend, far2, near2,
    in_sem, zs, zr, ss, sr, ps, pr, xs, xr, fs, fr,
):
    z, y, c, x = (lax.axis_index(a) for a in AXES)
    p = x * (1 - c) + y * c
    q = y * (1 - c) + x * c

    def at_z(zz):
        return {"z": zz, "y": y, "c": c, "x": x}

    def at_pq(pp, qq):
        return {"z": z, "y": qq * (1 - c) + pp * c, "c": c, "x": pp * (1 - c) + qq * c}

    def zmod(d):
        return lax.rem(z + (d + NZ), NZ)

    def pmod(d):
        return lax.rem(p + (d + 4), 4)

    def qmod(d):
        return lax.rem(q + (d + 4), 4)

    sibling = {"z": z, "y": y, "c": 1 - c, "x": x}
    pending = []

    def send(src, dst, ssem, rsem, dev):
        copy = pltpu.make_async_remote_copy(
            src_ref=src, dst_ref=dst, send_sem=ssem, recv_sem=rsem,
            device_id=dev, device_id_type=pl.DeviceIdType.MESH,
        )
        copy.start()
        pending.append(copy)

    def arrived(ref, sem):
        pltpu.make_async_copy(ref, ref, sem).wait()

    own = q * 4 + p
    loads = (
        pltpu.make_async_copy(gen_ref, rows.at[own], in_sem.at[0]),
        pltpu.make_async_copy(gen_ref, cols.at[z, c, 0], in_sem.at[1]),
        pltpu.make_async_copy(real_ref, cols.at[z, c, 1], in_sem.at[2]),
    )
    for copy in loads:
        copy.start()
    barrier = pltpu.get_barrier_semaphore()
    near = (
        sibling, at_z(zmod(1)), at_z(zmod(-1)),
        at_pq(pmod(1), q), at_pq(pmod(-1), q), at_pq(p, qmod(1)), at_pq(p, qmod(-1)),
    )
    for dev in near:
        pl.semaphore_signal(barrier, inc=1, device_id=dev, device_id_type=pl.DeviceIdType.MESH)
    pl.semaphore_wait(barrier, len(near))
    for copy in loads:
        copy.wait()

    def z_send(d, h, kind):
        s = 1 - 2 * d
        src = cols.at[zmod(-s * (h - 1)), c, kind]
        k = (d * 4 + h - 1) * 2 + kind
        send(src, src, zs.at[k], zr.at[k], at_z(zmod(s)))

    def sib_send(d, h, kind):
        s = 1 - 2 * d
        src = cols.at[zmod(-s * h), c, kind]
        k = (d * 5 + h) * 2 + kind
        send(src, src, ss.at[k], sr.at[k], sibling)

    def z_arrive(h, turn):
        for d in (0, 1):
            s = 1 - 2 * d
            kind = d if turn == 0 else 1 - d
            if h == 4 and turn == 1:
                continue
            arrived(cols.at[zmod(-s * h), c, kind], zr.at[(d * 4 + h - 1) * 2 + kind])
            if h < 3 or (h == 3 and turn == 0):
                z_send(d, h + 1, kind)
            sib_send(d, h, kind)

    def sib_arrive(h):
        for d in (0, 1):
            s = 1 - 2 * d
            if h == 0 and d == 1:
                continue
            for kind in (0, 1):
                if h == 4 and kind != d:
                    continue
                arrived(cols.at[zmod(-s * h), 1 - c, kind], sr.at[(d * 5 + h) * 2 + kind])

    for turn in (0, 1):
        for d in (0, 1):
            z_send(d, 1, d if turn == 0 else 1 - d)
    send(rows.at[own], rows.at[own], ps.at[0], pr.at[0], at_pq(pmod(1), q))
    send(rows.at[own], rows.at[own], ps.at[1], pr.at[1], at_pq(pmod(-1), q))
    sib_send(0, 0, 0)
    sib_send(0, 0, 1)

    left, right = q * 4 + pmod(-1), q * 4 + pmod(1)
    far = q * 4 + pmod(2)
    arrived(rows.at[left], pr.at[0])
    top = rows.at[left, pl.ds(0, 16)]
    send(top, top, ps.at[2], pr.at[2], at_pq(pmod(1), q))
    arrived(rows.at[right], pr.at[1])
    low = rows.at[right, pl.ds(16, 16)]
    send(low, low, ps.at[3], pr.at[3], at_pq(pmod(-1), q))
    z_arrive(1, 0)
    arrived(rows.at[far, pl.ds(0, 16)], pr.at[2])
    arrived(rows.at[far, pl.ds(16, 16)], pr.at[3])
    mine = rows.at[pl.ds(q * 4, 4)]
    send(mine, mine, ps.at[4], pr.at[4], at_pq(p, qmod(1)))
    send(mine, mine, ps.at[5], pr.at[5], at_pq(p, qmod(-1)))
    z_arrive(1, 1)
    z_arrive(2, 0)

    def squares_of(value):
        value = value.astype(F32)
        return jnp.sum(value * value, axis=1, keepdims=True)

    def row_squares(qq):
        def one(k, carry):
            g = qq * 4 + k
            rsq[pl.ds(g * PER, PER), :] = squares_of(rows[g])
            return carry
        lax.fori_loop(0, 4, one, 0)

    def col_squares(zz):
        total = to_lanes(squares_of(cols[zz].reshape(CHUNK, WIDTH)))
        csv[pl.ds(zz, 1), :] = total

    row_squares(q)
    z_arrive(2, 1)
    before, after, across = qmod(-1), qmod(1), qmod(2)
    arrived(rows.at[pl.ds(before * 4, 4)], pr.at[4])
    top = rows.at[pl.ds(before * 4, 2)]
    send(top, top, ps.at[6], pr.at[6], at_pq(p, after))
    arrived(rows.at[pl.ds(after * 4, 4)], pr.at[5])
    low = rows.at[pl.ds(after * 4 + 2, 2)]
    send(low, low, ps.at[7], pr.at[7], at_pq(p, before))
    row_squares(before)
    row_squares(after)
    sib_arrive(0)
    sib_arrive(1)
    sib_arrive(2)
    for d in (0, 1, -1):
        col_squares(zmod(d))
    z_arrive(3, 0)
    col_squares(zmod(2))
    col_squares(zmod(-2))
    arrived(rows.at[pl.ds(across * 4, 2)], pr.at[6])
    arrived(rows.at[pl.ds(across * 4 + 2, 2)], pr.at[7])
    row_squares(across)

    def tile(za, zb):
        rhs = jnp.concatenate(
            [cols[za].reshape(CHUNK, WIDTH), cols[zb].reshape(CHUNK, WIDTH)], axis=0
        )
        inner = lax.dot_general(
            rows[...].reshape(ROWS, WIDTH), rhs, (((1,), (1,)), ((), ())),
            preferred_element_type=F32,
        )
        for k, zz in enumerate((za, zb)):
            gap = rsq[...] + csv[pl.ds(zz, 1), :] - 2.0 * inner[:, k * CHUNK : (k + 1) * CHUNK]
            lane = pl.ds(pl.multiple_of(zz * CHUNK, CHUNK), CHUNK)
            logits[:, lane] = -jnp.sqrt(jnp.maximum(gap, 1.0)) * INV_SCALE

    def column_stats(zz):
        lane = pl.ds(pl.multiple_of(zz * CHUNK, CHUNK), CHUNK)
        block = logits[:, lane]
        peak = jnp.max(block, axis=0, keepdims=True)
        total = jnp.sum(jnp.exp(block - peak), axis=0, keepdims=True)
        cstat[z * NC + c, pl.ds(zz, 1), :] = peak + jnp.log(total)

    tile(zmod(-1), zmod(1))
    column_stats(zmod(-1))
    column_stats(zmod(1))
    z_arrive(3, 1)
    tile(zmod(-2), zmod(2))
    column_stats(zmod(-2))
    column_stats(zmod(2))
    sib_arrive(3)
    col_squares(zmod(-3))
    col_squares(zmod(3))
    tile(zmod(-3), zmod(3))
    column_stats(zmod(-3))
    column_stats(zmod(3))
    z_arrive(4, 0)
    sib_arrive(4)
    col_squares(zmod(4))
    tile(z, zmod(4))
    mine_rows = pl.ds(pl.multiple_of(own * PER, PER), PER)
    mine_lanes = pl.ds(pl.multiple_of(z * CHUNK, CHUNK), CHUNK)
    block = logits[mine_rows, mine_lanes]
    lane_id = lax.broadcasted_iota(jnp.int32, block.shape, 1)
    row_id = lax.broadcasted_iota(jnp.int32, block.shape, 0)
    logits[mine_rows, mine_lanes] = jnp.where(lane_id == row_id + c * 64, MASKED, block)
    column_stats(z)
    column_stats(zmod(4))

    def exchange(buf, me, peer_of, k):
        def one(t, carry):
            there = lax.rem(me + t, 16)
            pltpu.make_async_remote_copy(
                src_ref=buf.at[me], dst_ref=buf.at[me], send_sem=xs.at[k], recv_sem=xr.at[k],
                device_id=peer_of(there), device_id_type=pl.DeviceIdType.MESH,
            ).start()
            return carry
        lax.fori_loop(1, 16, one, 0)

    def exchanged(buf, k):
        some = buf.at[pl.ds(0, 15)]
        pltpu.make_async_copy(some, some, xr.at[k]).wait()

    def z_peer(k):
        return {"z": k // 2, "y": y, "c": lax.rem(k, 2), "x": x}

    def pq_peer(k):
        return at_pq(lax.rem(k, 4), k // 4)

    zc = z * NC + c
    exchange(cstat, zc, z_peer, 0)

    def row_stats(k, carry):
        part = pl.ds(pl.multiple_of(k * 128, 128), 128)
        block = logits[part, :]
        peak = jnp.max(block, axis=1, keepdims=True)
        total = jnp.sum(jnp.exp(block - peak), axis=1, keepdims=True)
        rstat[own, pl.ds(k, 1), :] = to_lanes(peak + jnp.log(total))
        return carry

    lax.fori_loop(0, 4, row_stats, 0)
    exchange(rstat, own, pq_peer, 1)

    def joined(buf):
        peak = buf[0]
        for k in range(1, 16):
            peak = jnp.maximum(peak, buf[k])
        total = jnp.exp(buf[0] - peak)
        for k in range(1, 16):
            total = total + jnp.exp(buf[k] - peak)
        return peak + jnp.log(total)

    exchanged(cstat, 0)
    csv[...] = 0.5 * joined(cstat)
    exchanged(rstat, 1)
    rall = 0.5 * joined(rstat)
    for k in range(4):
        rvec[pl.ds(k * 128, 128), :] = to_rows(rall[k : k + 1, :])
    is_real = lax.rem(lax.broadcasted_iota(jnp.int32, (1, COLS), 1) // PER, 2) == 1

    def halves(k, carry):
        part = pl.ds(pl.multiple_of(k * 128, 128), 128)
        shift = jnp.concatenate([csv[j : j + 1, :] for j in range(NZ)], axis=1)
        half = jnp.exp(logits[part, :] - rvec[part, :] - shift)
        logits[part, :] = half
        real = jnp.sum(jnp.where(is_real, half, 0.0), axis=1, keepdims=True)
        gen = jnp.sum(jnp.where(is_real, 0.0, half), axis=1, keepdims=True)
        mstat[own, pl.ds(k, 1), :] = to_lanes(gen)
        mstat[own, pl.ds(4 + k, 1), :] = to_lanes(real)
        return carry

    lax.fori_loop(0, 4, halves, 0)
    exchange(mstat, own, pq_peer, 2)
    exchanged(mstat, 2)
    mass = mstat[0]
    for k in range(1, 16):
        mass = mass + mstat[k]
    for k in range(4):
        gvec[pl.ds(k * 128, 128), :] = to_rows(mass[k : k + 1, :])
        mvec[pl.ds(k * 128, 128), :] = -to_rows(mass[k + 4 : k + 5, :])

    def drift(qq):
        part = pl.ds(pl.multiple_of(qq * 128, 128), 128)
        scale = jnp.where(is_real, gvec[part, :], mvec[part, :])
        weights = (logits[part, :] * scale).astype(BF16)
        return jnp.dot(weights, cols[...].reshape(COLS, WIDTH), preferred_element_type=F32)

    ahead, behind = at_pq(p, after), at_pq(p, before)
    part = drift(across).reshape(4, PER, WIDTH)
    psend[across] = part.astype(BF16)
    send(psend.at[across, pl.ds(0, 2)], far1.at[0], fs.at[0], fr.at[0], ahead)
    send(psend.at[across, pl.ds(2, 2)], far1.at[1], fs.at[1], fr.at[1], behind)
    part = drift(after).reshape(4, PER, WIDTH)
    psend[after, 2:4] = part[2:4].astype(BF16)
    send(psend.at[after, pl.ds(2, 2)], near1.at[0, pl.ds(2, 2)], fs.at[2], fr.at[2], ahead)
    acc[0:2] = part[0:2]
    part = drift(before).reshape(4, PER, WIDTH)
    psend[before, 0:2] = part[0:2].astype(BF16)
    send(psend.at[before, pl.ds(0, 2)], near1.at[1, pl.ds(0, 2)], fs.at[3], fr.at[3], behind)
    acc[2:4] = part[2:4]
    arrived(far1.at[0], fr.at[0])
    psend[after, 0:2] = (acc[0:2] + far1[0].astype(F32)).astype(BF16)
    send(psend.at[after, pl.ds(0, 2)], near1.at[0, pl.ds(0, 2)], fs.at[4], fr.at[4], ahead)
    arrived(far1.at[1], fr.at[1])
    psend[before, 2:4] = (acc[2:4] + far1[1].astype(F32)).astype(BF16)
    send(psend.at[before, pl.ds(2, 2)], near1.at[1, pl.ds(2, 2)], fs.at[5], fr.at[5], behind)
    acc[...] = drift(q).reshape(4, PER, WIDTH)
    arrived(near1.at[0, pl.ds(2, 2)], fr.at[2])
    arrived(near1.at[1, pl.ds(0, 2)], fr.at[3])
    arrived(near1.at[0, pl.ds(0, 2)], fr.at[4])
    arrived(near1.at[1, pl.ds(2, 2)], fr.at[5])

    def summed(k):
        return acc[k] + near1[0, k].astype(F32) + near1[1, k].astype(F32)

    ahead, behind = at_pq(pmod(1), q), at_pq(pmod(-1), q)
    qsend[2] = summed(pmod(2)).astype(BF16)
    send(qsend.at[2, pl.ds(0, 16)], far2.at[0], fs.at[6], fr.at[6], ahead)
    send(qsend.at[2, pl.ds(16, 16)], far2.at[1], fs.at[7], fr.at[7], behind)
    part = summed(pmod(1))
    qsend[1, 16:32] = part[16:32].astype(BF16)
    send(qsend.at[1, pl.ds(16, 16)], near2.at[0, pl.ds(16, 16)], fs.at[8], fr.at[8], ahead)
    hold_a = part[0:16]
    part = summed(pmod(-1))
    qsend[3, 0:16] = part[0:16].astype(BF16)
    send(qsend.at[3, pl.ds(0, 16)], near2.at[1, pl.ds(0, 16)], fs.at[9], fr.at[9], behind)
    hold_b = part[16:32]
    arrived(far2.at[0], fr.at[6])
    qsend[1, 0:16] = (hold_a + far2[0].astype(F32)).astype(BF16)
    send(qsend.at[1, pl.ds(0, 16)], near2.at[0, pl.ds(0, 16)], fs.at[10], fr.at[10], ahead)
    arrived(far2.at[1], fr.at[7])
    qsend[3, 16:32] = (hold_b + far2[1].astype(F32)).astype(BF16)
    send(qsend.at[3, pl.ds(16, 16)], near2.at[1, pl.ds(16, 16)], fs.at[11], fr.at[11], behind)
    raw = summed(p)
    arrived(near2.at[0, pl.ds(16, 16)], fr.at[8])
    arrived(near2.at[1, pl.ds(0, 16)], fr.at[9])
    arrived(near2.at[0, pl.ds(0, 16)], fr.at[10])
    arrived(near2.at[1, pl.ds(16, 16)], fr.at[11])
    raw = raw + near2[0].astype(F32) + near2[1].astype(F32)
    out_ref[...] = raw
    n1[zc] = jnp.broadcast_to(jnp.sum(raw * raw, keepdims=True), (8, 128))
    exchange(n1, zc, z_peer, 3)
    exchanged(n1, 3)
    total = n1[0]
    for k in range(1, 16):
        total = total + n1[k]
    n2[own] = total
    exchange(n2, own, pq_peer, 4)
    exchanged(n2, 4)
    total = n2[0]
    for k in range(1, 16):
        total = total + n2[k]
    scale = lax.rsqrt(total[0:1, 0:1] / (NX * NY * NZ * NC * PER * WIDTH) + EPS)
    out_ref[...] = out_ref[...] * scale

    for copy in pending:
        copy.wait_send()
    for k, buf in enumerate((cstat, rstat, mstat, n1, n2)):
        some = buf.at[pl.ds(0, 15)]
        pltpu.make_async_copy(some, some, xs.at[k]).wait()


def on_device(gen, real):
    dma = pltpu.SemaphoreType.DMA
    return pl.pallas_call(
        kernel,
        out_shape=jax.ShapeDtypeStruct((PER, WIDTH), F32),
        in_specs=[pl.BlockSpec(memory_space=pl.ANY)] * 2,
        out_specs=pl.BlockSpec(memory_space=pltpu.VMEM),
        scratch_shapes=[
            pltpu.VMEM((16, PER, WIDTH), BF16),
            pltpu.VMEM((NZ, NC, 2, PER, WIDTH), BF16),
            pltpu.VMEM((ROWS, COLS), F32),
            pltpu.VMEM((8, 128), BF16),
            pltpu.VMEM((ROWS, 1), F32),
            pltpu.VMEM((ROWS, 1), F32),
            pltpu.VMEM((ROWS, 1), F32),
            pltpu.VMEM((ROWS, 1), F32),
            pltpu.VMEM((NZ, CHUNK), F32),
            pltpu.VMEM((16, NZ, CHUNK), F32),
            pltpu.VMEM((16, 4, 128), F32),
            pltpu.VMEM((16, 8, 128), F32),
            pltpu.VMEM((16, 8, 128), F32),
            pltpu.VMEM((16, 8, 128), F32),
            pltpu.VMEM((4, 4, PER, WIDTH), BF16),
            pltpu.VMEM((4, PER, WIDTH), F32),
            pltpu.VMEM((2, 2, PER, WIDTH), BF16),
            pltpu.VMEM((2, 4, PER, WIDTH), BF16),
            pltpu.VMEM((4, PER, WIDTH), BF16),
            pltpu.VMEM((2, PER // 2, WIDTH), BF16),
            pltpu.VMEM((2, PER, WIDTH), BF16),
            dma((3,)), dma((16,)), dma((16,)), dma((20,)), dma((20,)),
            dma((8,)), dma((8,)), dma((5,)), dma((5,)), dma((12,)), dma((12,)),
        ],
        compiler_params=pltpu.CompilerParams(
            collective_id=0, has_side_effects=True, vmem_limit_bytes=60 * 1024 * 1024
        ),
    )(gen, real)


def solution(mesh):
    torus = Mesh(mesh.devices.reshape(NZ, NY, NC, NX), AXES)
    return jax.shard_map(
        on_device,
        mesh=torus,
        in_specs=(P(AXES, None), P(AXES, None)),
        out_specs=P(AXES, None),
        check_vma=False,
    )
```

```python
import jax
import jax.numpy as jnp
from jax import lax
from jax.experimental import pallas as pl
from jax.experimental.pallas import tpu as pltpu
from jax.sharding import Mesh
from jax.sharding import PartitionSpec as P

AXES = ("z", "y", "c", "x")
NZ, NY, NC, NX = 8, 4, 2, 4
PER = 32
HALF = PER // 2
WIDTH = 2048
ROWS = NX * NY * PER
CHUNK = 2 * NC * PER
COLS = NZ * CHUNK
SLICES = 4
PIECE = WIDTH // SLICES
INV_SCALE = 1.0 / 0.3
MASKED = -1e30
EPS = 1e-6
F32 = jnp.float32
BF16 = jnp.bfloat16
MESH = pl.DeviceIdType.MESH
SEMS = 128


def eye():
    return lax.broadcasted_iota(jnp.int32, (128, 128), 0) == lax.broadcasted_iota(
        jnp.int32, (128, 128), 1
    )


def to_lanes(v):
    return jnp.sum(jnp.where(eye(), jnp.broadcast_to(v, (128, 128)), 0.0), axis=0, keepdims=True)


def to_rows(v):
    return jnp.sum(jnp.where(eye(), jnp.broadcast_to(v, (128, 128)), 0.0), axis=1, keepdims=True)


def kernel(
    gen_ref, real_ref, raw_ref, norm_ref,
    rows, cols, logits, rsq, rvec, csq, cown, raw,
    cstat, rstat, mstat, n1, n2,
    weights, psend, acc, kept, far, near, qsend, qrecv,
    in_sem, out_sem, ssem, rsem, xs, xr,
):
    z, y, c, x = (lax.axis_index(a) for a in AXES)
    p = x * (1 - c) + y * c
    q = y * (1 - c) + x * c

    def at_z(zz, cc=c):
        return {"z": zz, "y": y, "c": cc, "x": x}

    def at_pq(pp, qq):
        return {"z": z, "y": qq * (1 - c) + pp * c, "c": c, "x": pp * (1 - c) + qq * c}

    def zmod(d):
        return lax.rem(z + (d + NZ), NZ)

    def pmod(d):
        return lax.rem(p + (d + 4), 4)

    def qmod(d):
        return lax.rem(q + (d + 4), 4)

    sibling = at_z(z, 1 - c)
    pending, used, index = [], [], {}

    def drain():
        for copy in pending:
            copy.wait_send()
        for k, buf in used:
            some = buf.at[pl.ds(0, 15)]
            pltpu.make_async_copy(some, some, xs.at[k]).wait()

    def send(key, src, dst, dev):
        k = index.setdefault(key, len(index))
        assert k == len(index) - 1 and k < SEMS
        copy = pltpu.make_async_remote_copy(
            src_ref=src, dst_ref=dst, send_sem=ssem.at[k], recv_sem=rsem.at[k],
            device_id=dev, device_id_type=MESH,
        )
        copy.start()
        pending.append(copy)

    def arrived(key, ref):
        pltpu.make_async_copy(ref, ref, rsem.at[index[key]]).wait()

    own = q * 4 + p
    loads = (
        pltpu.make_async_copy(gen_ref, rows.at[own], in_sem.at[0]),
        pltpu.make_async_copy(gen_ref, cols.at[z, c, 0], in_sem.at[1]),
        pltpu.make_async_copy(real_ref, cols.at[z, c, 1], in_sem.at[2]),
    )
    for copy in loads:
        copy.start()
    barrier = pltpu.get_barrier_semaphore()
    around = (
        sibling, at_z(zmod(1)), at_z(zmod(-1)),
        at_pq(pmod(1), q), at_pq(pmod(-1), q), at_pq(p, qmod(1)), at_pq(p, qmod(-1)),
    )
    for dev in around:
        pl.semaphore_signal(barrier, inc=1, device_id=dev, device_id_type=MESH)
    pl.semaphore_wait(barrier, len(around))
    for copy in loads:
        copy.wait()

    top, low = pl.ds(0, HALF), pl.ds(HALF, HALF)

    def z_piece(d, h, j):
        kind = j // 2 if d == 0 else 1 - j // 2
        return cols.at[zmod((2 * d - 1) * h), c, kind, low if j % 2 else top], kind

    def z_send(d, h, j):
        src, _ = z_piece(d, h - 1, j)
        send(("z", d, h, j), src, src, at_z(zmod(1 - 2 * d)))

    def z_arrive(h, j):
        for d in (0, 1):
            src, kind = z_piece(d, h, j)
            arrived(("z", d, h, j), src)
            if h < 3 or (h == 3 and j < 2):
                z_send(d, h + 1, j)
            if h == 4:
                send(("s", d, h, j), src, src, sibling)
            elif j % 2:
                whole = cols.at[zmod((2 * d - 1) * h), c, kind]
                send(("s", d, h, kind), whole, whole, sibling)

    def sib_arrive(h):
        for d in (0, 1):
            zz = zmod((2 * d - 1) * h)
            if h == 4:
                for j in (0, 1):
                    arrived(("s", d, h, j), cols.at[zz, 1 - c, d, low if j else top])
            elif h or not d:
                for kind in (0, 1):
                    arrived(("s", d, h, kind), cols.at[zz, 1 - c, kind])

    def at_row(dq, dp):
        return qmod(dq) * 4 + pmod(dp)

    def q_sends(dp):
        block = rows.at[at_row(0, dp)]
        send(("q", 1, dp), block, block, at_pq(p, qmod(1)))
        send(("q", -1, dp), block, block, at_pq(p, qmod(-1)))

    def p_arrive(d):
        arrived(("p", d), rows.at[at_row(0, -d)])
        half = rows.at[at_row(0, -d), top if d > 0 else low]
        send(("pf", d), half, half, at_pq(pmod(d), q))
        q_sends(-d)

    def p_far():
        arrived(("pf", 1), rows.at[at_row(0, 2), top])
        arrived(("pf", -1), rows.at[at_row(0, 2), low])
        q_sends(2)

    def q_arrive(dp):
        for d in (1, -1):
            arrived(("q", d, dp), rows.at[at_row(-d, dp)])
            half = rows.at[at_row(-d, dp), top if d > 0 else low]
            send(("qf", d, dp), half, half, at_pq(p, qmod(d)))

    def q_far(dp):
        arrived(("qf", 1, dp), rows.at[at_row(2, dp), top])
        arrived(("qf", -1, dp), rows.at[at_row(2, dp), low])

    def squares_of(value):
        value = value.astype(F32)
        return jnp.sum(value * value, axis=1, keepdims=True)

    def row_squares(dq):
        def one(k, carry):
            g = qmod(dq) * 4 + k
            rsq[pl.ds(g * PER, PER), :] = jnp.broadcast_to(squares_of(rows[g]), (PER, CHUNK))
            return carry
        lax.fori_loop(0, 4, one, 0)

    def col_squares(d):
        csq[pl.ds(zmod(d), 1), :] = to_lanes(squares_of(cols[zmod(d)].reshape(CHUNK, WIDTH)))

    def lanes_of(d):
        return pl.ds(pl.multiple_of(zmod(d) * CHUNK, CHUNK), CHUNK)

    zc = z * NC + c

    def tile(*ds):
        rhs = [cols[zmod(d)].reshape(CHUNK, WIDTH) for d in ds]
        rhs = jnp.concatenate(rhs, axis=0) if len(rhs) > 1 else rhs[0]
        inner = lax.dot_general(
            rows[...].reshape(ROWS, WIDTH), rhs, (((1,), (1,)), ((), ())),
            preferred_element_type=F32,
        )
        for k, d in enumerate(ds):
            gap = rsq[...] + csq[pl.ds(zmod(d), 1), :] - 2.0 * inner[:, k * CHUNK : (k + 1) * CHUNK]
            gap = jnp.maximum(gap, 1.0)
            logits[:, lanes_of(d)] = gap * lax.rsqrt(gap) * -INV_SCALE
        if ds == (0,):
            mine = pl.ds(pl.multiple_of(own * PER, PER), PER)
            block = logits[mine, lanes_of(0)]
            lane_id = lax.broadcasted_iota(jnp.int32, block.shape, 1)
            row_id = lax.broadcasted_iota(jnp.int32, block.shape, 0)
            logits[mine, lanes_of(0)] = jnp.where(lane_id == row_id + c * 2 * PER, MASKED, block)
        for d in ds:
            block = logits[:, lanes_of(d)]
            peak = jnp.max(block, axis=0, keepdims=True)
            total = jnp.sum(jnp.exp(block - peak), axis=0, keepdims=True)
            cstat[zc, pl.ds(zmod(d), 1), :] = peak + jnp.log(total)

    for j in range(4):
        for d in (0, 1):
            z_send(d, 1, j)
    for d in (1, -1):
        send(("p", d), rows.at[own], rows.at[own], at_pq(pmod(d), q))
    q_sends(0)
    for kind in (0, 1):
        send(("s", 0, 0, kind), cols.at[z, c, kind], cols.at[z, c, kind], sibling)

    events = []

    def plan(when, what, *args):
        events.append((when, len(events), what, args))

    for h in range(1, 5):
        for j in range(4 if h < 4 else 2):
            plan(3.0 + 1.4 * ((h - 1) * 4 + j + 1), z_arrive, h, j)
    plan(4.3, p_arrive, 1)
    plan(4.3, p_arrive, -1)
    plan(5.9, q_arrive, 0)
    plan(8.1, p_far)
    plan(9.2, q_arrive, -1)
    plan(10.2, q_arrive, 1)
    plan(12.5, q_arrive, 2)
    plan(9.9, q_far, 0)
    plan(13.0, q_far, -1)
    plan(14.0, q_far, 1)
    plan(16.3, q_far, 2)
    plan(6.0, sib_arrive, 0)
    plan(6.0, col_squares, 0)
    plan(8.2, row_squares, 0)
    plan(12.6, sib_arrive, 1)
    plan(12.6, col_squares, 1)
    plan(13.1, col_squares, -1)
    plan(14.3, row_squares, 1)
    plan(14.6, row_squares, -1)
    plan(16.4, row_squares, 2)
    plan(16.5, tile, 0)
    plan(17.1, tile, 1, -1)
    plan(18.5, sib_arrive, 2)
    plan(18.5, col_squares, 2)
    plan(18.6, col_squares, -2)
    plan(19.9, tile, 2, -2)
    plan(22.61, sib_arrive, 3)
    plan(22.62, col_squares, 3)
    plan(22.63, col_squares, -3)
    plan(22.64, tile, 3, -3)
    for _, _, what, args in sorted(events, key=lambda e: e[:2]):
        what(*args)
    sib_arrive(4)
    col_squares(4)
    tile(4)

    z_order = [(d, k) for d in (4, 3, -3, 2, -2, 1, -1, 0) for k in (1, 0) if d or k]
    pq_order = sorted(
        ((i, j) for i in range(4) for j in range(4) if i or j),
        key=lambda d: -min(d[0], 4 - d[0]) - min(d[1], 4 - d[1]),
    )
    z_peers = [at_z(zmod(d), c + k - 2 * c * k) for d, k in z_order]
    pq_peers = [at_pq(pmod(i), qmod(j)) for i, j in pq_order]

    def exchange(buf, me, peers):
        k = len(used)
        for dev in peers:
            pltpu.make_async_remote_copy(
                src_ref=buf.at[me], dst_ref=buf.at[me], send_sem=xs.at[k], recv_sem=xr.at[k],
                device_id=dev, device_id_type=MESH,
            ).start()
        used.append((k, buf))

        def wait():
            some = buf.at[pl.ds(0, 15)]
            pltpu.make_async_copy(some, some, xr.at[k]).wait()

        return wait

    def joined(buf):
        peak = buf[0]
        for k in range(1, 16):
            peak = jnp.maximum(peak, buf[k])
        total = jnp.exp(buf[0] - peak)
        for k in range(1, 16):
            total = total + jnp.exp(buf[k] - peak)
        return peak + jnp.log(total)

    def in_line(v):
        return jnp.concatenate([v[j : j + 1, :] for j in range(NZ)], axis=1)

    columns_known = exchange(cstat, zc, z_peers)
    cown[...] = cstat[zc]

    def row_stats(k, carry):
        part = pl.ds(pl.multiple_of(k * 128, 128), 128)
        block = logits[part, :]
        peak = jnp.max(block, axis=1, keepdims=True)
        total = peak + jnp.log(jnp.sum(jnp.exp(block - peak), axis=1, keepdims=True))
        rvec[part, :] = 0.5 * total
        rstat[own, pl.ds(k, 1), :] = to_lanes(total)
        return carry

    lax.fori_loop(0, 4, row_stats, 0)
    rows_known = exchange(rstat, own, pq_peers)

    def start_halves(k, carry):
        part = pl.ds(pl.multiple_of(k * 128, 128), 128)
        logits[part, :] = jnp.exp(logits[part, :] - rvec[part, :] - 0.5 * in_line(cown[...]))
        return carry

    lax.fori_loop(0, 4, start_halves, 0)
    columns_known()
    cown[...] = jnp.exp(0.5 * (cown[...] - joined(cstat)))
    lane_id = lax.broadcasted_iota(jnp.int32, (1, CHUNK), 1)
    is_real = lax.rem(lane_id // PER, 2) == 1

    def masses(k, carry):
        part = pl.ds(pl.multiple_of(k * 128, 128), 128)
        total = logits[part, 0:CHUNK] * cown[0:1, :]
        for j in range(1, NZ):
            total = total + logits[part, j * CHUNK : (j + 1) * CHUNK] * cown[j : j + 1, :]
        real = jnp.sum(jnp.where(is_real, total, 0.0), axis=1, keepdims=True)
        gen = jnp.sum(jnp.where(is_real, 0.0, total), axis=1, keepdims=True)
        mstat[own, pl.ds(k, 1), :] = to_lanes(gen)
        mstat[own, pl.ds(4 + k, 1), :] = to_lanes(real)
        return carry

    lax.fori_loop(0, 4, masses, 0)
    masses_known = exchange(mstat, own, pq_peers)
    rows_known()
    joint = joined(rstat)
    shares = [jnp.exp(0.5 * (rstat[k] - joint)) for k in range(16)]
    my_share = jnp.exp(0.5 * (rstat[own] - joint))
    masses_known()
    gen = shares[0] * mstat[0, 0:4]
    real = shares[0] * mstat[0, 4:8]
    for k in range(1, 16):
        gen = gen + shares[k] * mstat[k, 0:4]
        real = real + shares[k] * mstat[k, 4:8]
    mstat[16, 0:4] = my_share * gen
    mstat[16, 4:8] = -my_share * real

    def weigh(qq, at):
        part = pl.ds(pl.multiple_of(qq * 128, 128), 128)
        on_real = to_rows(mstat[16, pl.ds(qq, 1), :])
        on_gen = to_rows(mstat[16, pl.ds(qq + 4, 1), :])
        scale = jnp.where(is_real, on_real, on_gen)
        for j in range(NZ):
            half = logits[part, j * CHUNK : (j + 1) * CHUNK] * cown[j : j + 1, :]
            weights[at, :, j * CHUNK : (j + 1) * CHUNK] = (half * scale).astype(BF16)

    def drift(w, s):
        samples = cols[:, :, :, :, s * PIECE : (s + 1) * PIECE].reshape(COLS, PIECE)
        return jnp.dot(w, samples, preferred_element_type=F32)

    before, after, across = qmod(-1), qmod(1), qmod(2)
    ahead, behind = at_pq(p, after), at_pq(p, before)
    lo, hi = pl.ds(0, 2), pl.ds(2, 2)
    weigh(across, 0)
    for s in range(SLICES):
        psend[s, 0] = drift(weights[0], s).reshape(4, PER, PIECE).astype(BF16)
        send(("f", 1, s), psend.at[s, 0, lo], far.at[s, 0], ahead)
        send(("f", -1, s), psend.at[s, 0, hi], far.at[s, 1], behind)
    weigh(after, 1)
    weigh(before, 2)
    for s in range(SLICES):
        part = drift(weights[1:3].reshape(256, COLS), s).reshape(8, PER, PIECE)
        psend[s, 1, 2:4] = part[2:4].astype(BF16)
        send(("i", 1, s), psend.at[s, 1, hi], near.at[s, 0, hi], ahead)
        psend[s, 2, 0:2] = part[4:6].astype(BF16)
        send(("i", -1, s), psend.at[s, 2, lo], near.at[s, 1, lo], behind)
        kept[s, 0:2] = part[0:2]
        kept[s, 2:4] = part[6:8]
    weigh(q, 0)
    for s in range(SLICES):
        acc[s] = drift(weights[0], s).reshape(4, PER, PIECE)
    for s in range(SLICES):
        arrived(("f", 1, s), far.at[s, 0])
        psend[s, 1, 0:2] = (kept[s, 0:2] + far[s, 0].astype(F32)).astype(BF16)
        send(("d", 1, s), psend.at[s, 1, lo], near.at[s, 0, lo], ahead)
        arrived(("f", -1, s), far.at[s, 1])
        psend[s, 2, 2:4] = (kept[s, 2:4] + far[s, 1].astype(F32)).astype(BF16)
        send(("d", -1, s), psend.at[s, 2, hi], near.at[s, 1, hi], behind)
    for s in range(SLICES):
        arrived(("i", 1, s), near.at[s, 0, hi])
        arrived(("i", -1, s), near.at[s, 1, lo])
        arrived(("d", 1, s), near.at[s, 0, lo])
        arrived(("d", -1, s), near.at[s, 1, hi])
        for d in (2, 1, 3):
            k = pmod(d)
            total = acc[s, k] + near[s, 0, k].astype(F32) + near[s, 1, k].astype(F32)
            qsend[s, d - 1] = total.astype(BF16)
            send(("r", d, s), qsend.at[s, d - 1], qrecv.at[s, d - 1], at_pq(k, q))
    square = jnp.zeros((PER, 128), F32)
    for s in range(SLICES):
        total = acc[s, p] + near[s, 0, p].astype(F32) + near[s, 1, p].astype(F32)
        for d in (1, 3, 2):
            arrived(("r", d, s), qrecv.at[s, d - 1])
            total = total + qrecv[s, d - 1].astype(F32)
        raw[:, s * PIECE : (s + 1) * PIECE] = total
        for k in range(PIECE // 128):
            lane = total[:, k * 128 : (k + 1) * 128]
            square = square + lane * lane
    n1[zc] = jnp.broadcast_to(jnp.sum(square, keepdims=True), (1, 128))
    first_known = exchange(n1, zc, z_peers)
    out = pltpu.make_async_copy(raw, raw_ref, out_sem)
    out.start()
    first_known()
    total = n1[0]
    for k in range(1, 16):
        total = total + n1[k]
    n2[own] = total
    second_known = exchange(n2, own, pq_peers)
    out.wait()
    second_known()
    total = n2[0]
    for k in range(1, 16):
        total = total + n2[k]
    count = NX * NY * NZ * NC * PER * WIDTH
    norm_ref[0, 0] = lax.rsqrt(total / count + EPS)[0, 0]
    drain()


def on_device(gen, real):
    dma = pltpu.SemaphoreType.DMA
    raw, norm = pl.pallas_call(
        kernel,
        out_shape=(
            jax.ShapeDtypeStruct((PER, WIDTH), F32), jax.ShapeDtypeStruct((1, 1), F32),
        ),
        in_specs=[pl.BlockSpec(memory_space=pl.ANY)] * 2,
        out_specs=(
            pl.BlockSpec(memory_space=pl.ANY), pl.BlockSpec(memory_space=pltpu.SMEM),
        ),
        scratch_shapes=[
            pltpu.VMEM((16, PER, WIDTH), BF16),
            pltpu.VMEM((NZ, NC, 2, PER, WIDTH), BF16),
            pltpu.VMEM((ROWS, COLS), F32),
            pltpu.VMEM((ROWS, CHUNK), F32),
            pltpu.VMEM((ROWS, 1), F32),
            pltpu.VMEM((NZ, CHUNK), F32),
            pltpu.VMEM((NZ, CHUNK), F32),
            pltpu.VMEM((PER, WIDTH), F32),
            pltpu.VMEM((16, NZ, CHUNK), F32),
            pltpu.VMEM((16, 4, 128), F32),
            pltpu.VMEM((17, 8, 128), F32),
            pltpu.VMEM((16, 1, 128), F32),
            pltpu.VMEM((16, 1, 128), F32),
            pltpu.VMEM((3, 128, COLS), BF16),
            pltpu.VMEM((SLICES, 3, 4, PER, PIECE), BF16),
            pltpu.VMEM((SLICES, 4, PER, PIECE), F32),
            pltpu.VMEM((SLICES, 4, PER, PIECE), F32),
            pltpu.VMEM((SLICES, 2, 2, PER, PIECE), BF16),
            pltpu.VMEM((SLICES, 2, 4, PER, PIECE), BF16),
            pltpu.VMEM((SLICES, 3, PER, PIECE), BF16),
            pltpu.VMEM((SLICES, 3, PER, PIECE), BF16),
            dma((3,)), dma, dma((SEMS,)), dma((SEMS,)), dma((5,)), dma((5,)),
        ],
        compiler_params=pltpu.CompilerParams(
            collective_id=0, has_side_effects=True, vmem_limit_bytes=60 * 1024 * 1024
        ),
    )(gen, real)
    return raw * norm


def solution(mesh):
    torus = Mesh(mesh.devices.reshape(NZ, NY, NC, NX), AXES)
    return jax.shard_map(
        on_device,
        mesh=torus,
        in_specs=(P(AXES, None), P(AXES, None)),
        out_specs=P(AXES, None),
        check_vma=False,
    )
```

```python
import jax
import jax.numpy as jnp
from jax import lax
from jax.experimental import pallas as pl
from jax.experimental.pallas import tpu as pltpu
from jax.sharding import Mesh
from jax.sharding import PartitionSpec as P

AXES = ("z", "y", "c", "x")
NZ, NY, NC, NX = 8, 4, 2, 4
PER = 32
HALF = PER // 2
WIDTH = 2048
ROWS = NX * NY * PER
CHUNK = 2 * NC * PER
COLS = NZ * CHUNK
SLICES = 4
PIECE = WIDTH // SLICES
INV_SCALE = 1.0 / 0.3
MASKED = -1e30
EPS = 1e-6
F32 = jnp.float32
BF16 = jnp.bfloat16
MESH = pl.DeviceIdType.MESH
SEMS = 104


def eye():
    return lax.broadcasted_iota(jnp.int32, (128, 128), 0) == lax.broadcasted_iota(
        jnp.int32, (128, 128), 1
    )


def to_lanes(v):
    return jnp.sum(jnp.where(eye(), jnp.broadcast_to(v, (128, 128)), 0.0), axis=0, keepdims=True)


def to_rows(v):
    return jnp.sum(jnp.where(eye(), jnp.broadcast_to(v, (128, 128)), 0.0), axis=1, keepdims=True)


def kernel(
    gen_ref, real_ref, out_ref,
    rows, cols, logits, rsq, rvec, csq, cown,
    cstat, rstat, mstat, n1, n2,
    weights, psend, acc, kept, far, near, qsend, qrecv,
    in_sem, ssem, rsem, xs, xr,
):
    z, y, c, x = (lax.axis_index(a) for a in AXES)
    p = x * (1 - c) + y * c
    q = y * (1 - c) + x * c

    def at_z(zz, cc=c):
        return {"z": zz, "y": y, "c": cc, "x": x}

    def at_pq(pp, qq):
        return {"z": z, "y": qq * (1 - c) + pp * c, "c": c, "x": pp * (1 - c) + qq * c}

    def zmod(d):
        return lax.rem(z + (d + NZ), NZ)

    def pmod(d):
        return lax.rem(p + (d + 4), 4)

    def qmod(d):
        return lax.rem(q + (d + 4), 4)

    sibling = at_z(z, 1 - c)
    used, index = [], {}
    kinds = ("z", "s", "p", "f", "r")

    def drain():
        sent = (cols.at[pl.ds(0, 7), 0], cols.at[pl.ds(0, 8), 0], rows.at[pl.ds(0, 15)], psend, qsend)
        for k, ref in enumerate(sent):
            pltpu.make_async_copy(ref, ref, ssem.at[k]).wait()
        for k, buf in used:
            some = buf.at[pl.ds(0, 15)]
            pltpu.make_async_copy(some, some, xs.at[k]).wait()

    def send(key, src, dst, dev):
        k = index.setdefault(key, len(index))
        assert k == len(index) - 1 and k < SEMS
        kind = {"q": "p", "i": "f", "d": "f"}.get(key[0][0], key[0][0])
        pltpu.make_async_remote_copy(
            src_ref=src, dst_ref=dst, send_sem=ssem.at[kinds.index(kind)], recv_sem=rsem.at[k],
            device_id=dev, device_id_type=MESH,
        ).start()

    def arrived(key, ref):
        pltpu.make_async_copy(ref, ref, rsem.at[index[key]]).wait()

    own = q * 4 + p
    loads = (
        pltpu.make_async_copy(gen_ref, rows.at[own], in_sem.at[0]),
        pltpu.make_async_copy(gen_ref, cols.at[z, c, 0], in_sem.at[1]),
        pltpu.make_async_copy(real_ref, cols.at[z, c, 1], in_sem.at[2]),
    )
    for copy in loads:
        copy.start()
    barrier = pltpu.get_barrier_semaphore()
    around = (
        sibling, at_z(zmod(1)), at_z(zmod(-1)),
        at_pq(pmod(1), q), at_pq(pmod(-1), q), at_pq(p, qmod(1)), at_pq(p, qmod(-1)),
    )
    for dev in around:
        pl.semaphore_signal(barrier, inc=1, device_id=dev, device_id_type=MESH)
    pl.semaphore_wait(barrier, len(around))
    for copy in loads:
        copy.wait()

    top, low = pl.ds(0, HALF), pl.ds(HALF, HALF)

    def z_piece(d, h, j):
        kind = j // 2 if d == 0 else 1 - j // 2
        return cols.at[zmod((2 * d - 1) * h), c, kind, low if j % 2 else top], kind

    def z_send(d, h, j):
        src, _ = z_piece(d, h - 1, j)
        send(("z", d, h, j), src, src, at_z(zmod(1 - 2 * d)))

    def z_arrive(h, j):
        for d in (0, 1):
            src, kind = z_piece(d, h, j)
            arrived(("z", d, h, j), src)
            if h < 3 or (h == 3 and j < 2):
                z_send(d, h + 1, j)
            if h == 4:
                send(("s", d, h, j), src, src, sibling)
            elif j % 2:
                whole = cols.at[zmod((2 * d - 1) * h), c, kind]
                send(("s", d, h, kind), whole, whole, sibling)

    def sib_arrive(h):
        for d in (0, 1):
            zz = zmod((2 * d - 1) * h)
            if h == 4:
                for j in (0, 1):
                    arrived(("s", d, h, j), cols.at[zz, 1 - c, d, low if j else top])
            elif h or not d:
                for kind in (0, 1):
                    arrived(("s", d, h, kind), cols.at[zz, 1 - c, kind])

    def at_row(dq, dp):
        return qmod(dq) * 4 + pmod(dp)

    def q_sends(dp):
        block = rows.at[at_row(0, dp)]
        send(("q", 1, dp), block, block, at_pq(p, qmod(1)))
        send(("q", -1, dp), block, block, at_pq(p, qmod(-1)))

    def p_arrive(d):
        arrived(("p", d), rows.at[at_row(0, -d)])
        half = rows.at[at_row(0, -d), top if d > 0 else low]
        send(("pf", d), half, half, at_pq(pmod(d), q))
        q_sends(-d)

    def p_far():
        arrived(("pf", 1), rows.at[at_row(0, 2), top])
        arrived(("pf", -1), rows.at[at_row(0, 2), low])
        q_sends(2)

    def q_arrive(dp):
        for d in (1, -1):
            arrived(("q", d, dp), rows.at[at_row(-d, dp)])
            half = rows.at[at_row(-d, dp), top if d > 0 else low]
            send(("qf", d, dp), half, half, at_pq(p, qmod(d)))

    def q_far(dp):
        arrived(("qf", 1, dp), rows.at[at_row(2, dp), top])
        arrived(("qf", -1, dp), rows.at[at_row(2, dp), low])

    def squares_of(value):
        value = value.astype(F32)
        return jnp.sum(value * value, axis=1, keepdims=True)

    def row_squares(dq):
        def one(k, carry):
            g = qmod(dq) * 4 + k
            rsq[pl.ds(g * PER, PER), :] = jnp.broadcast_to(squares_of(rows[g]), (PER, CHUNK))
            return carry
        lax.fori_loop(0, 4, one, 0)

    def col_squares(d):
        csq[pl.ds(zmod(d), 1), :] = to_lanes(squares_of(cols[zmod(d)].reshape(CHUNK, WIDTH)))

    def lanes_of(d):
        return pl.ds(pl.multiple_of(zmod(d) * CHUNK, CHUNK), CHUNK)

    zc = z * NC + c

    def tile(*ds):
        rhs = [cols[zmod(d)].reshape(CHUNK, WIDTH) for d in ds]
        rhs = jnp.concatenate(rhs, axis=0) if len(rhs) > 1 else rhs[0]
        inner = lax.dot_general(
            rows[...].reshape(ROWS, WIDTH), rhs, (((1,), (1,)), ((), ())),
            preferred_element_type=F32,
        )
        for k, d in enumerate(ds):
            gap = rsq[...] + csq[pl.ds(zmod(d), 1), :] - 2.0 * inner[:, k * CHUNK : (k + 1) * CHUNK]
            gap = jnp.maximum(gap, 1.0)
            logits[:, lanes_of(d)] = gap * lax.rsqrt(gap) * -INV_SCALE
        if ds == (0,):
            mine = pl.ds(pl.multiple_of(own * PER, PER), PER)
            block = logits[mine, lanes_of(0)]
            lane_id = lax.broadcasted_iota(jnp.int32, block.shape, 1)
            row_id = lax.broadcasted_iota(jnp.int32, block.shape, 0)
            logits[mine, lanes_of(0)] = jnp.where(lane_id == row_id + c * 2 * PER, MASKED, block)
        for d in ds:
            block = logits[:, lanes_of(d)]
            peak = jnp.max(block, axis=0, keepdims=True)
            total = jnp.sum(jnp.exp(block - peak), axis=0, keepdims=True)
            cstat[zc, pl.ds(zmod(d), 1), :] = peak + jnp.log(total)

    for j in range(4):
        for d in (0, 1):
            z_send(d, 1, j)
    for d in (1, -1):
        send(("p", d), rows.at[own], rows.at[own], at_pq(pmod(d), q))
    q_sends(0)
    for kind in (0, 1):
        send(("s", 0, 0, kind), cols.at[z, c, kind], cols.at[z, c, kind], sibling)

    events = []

    def plan(when, what, *args):
        events.append((when, len(events), what, args))

    for h in range(1, 5):
        for j in range(4 if h < 4 else 2):
            plan(3.0 + 1.4 * ((h - 1) * 4 + j + 1), z_arrive, h, j)
    plan(4.3, p_arrive, 1)
    plan(4.3, p_arrive, -1)
    plan(5.9, q_arrive, 0)
    plan(8.1, p_far)
    plan(9.2, q_arrive, -1)
    plan(10.2, q_arrive, 1)
    plan(12.5, q_arrive, 2)
    plan(9.9, q_far, 0)
    plan(13.0, q_far, -1)
    plan(14.0, q_far, 1)
    plan(16.3, q_far, 2)
    plan(6.0, sib_arrive, 0)
    plan(6.0, col_squares, 0)
    plan(8.2, row_squares, 0)
    plan(12.6, sib_arrive, 1)
    plan(12.6, col_squares, 1)
    plan(13.1, col_squares, -1)
    plan(14.3, row_squares, 1)
    plan(14.6, row_squares, -1)
    plan(16.4, row_squares, 2)
    plan(16.5, tile, 0)
    plan(17.1, tile, 1, -1)
    plan(18.5, sib_arrive, 2)
    plan(18.5, col_squares, 2)
    plan(18.6, col_squares, -2)
    plan(19.9, tile, 2, -2)
    plan(22.61, sib_arrive, 3)
    plan(22.62, col_squares, 3)
    plan(22.63, col_squares, -3)
    plan(22.64, tile, 3, -3)
    for _, _, what, args in sorted(events, key=lambda e: e[:2]):
        what(*args)
    sib_arrive(4)
    col_squares(4)
    tile(4)

    z_order = [(d, k) for d in (4, 3, -3, 2, -2, 1, -1, 0) for k in (1, 0) if d or k]
    pq_order = sorted(
        ((i, j) for i in range(4) for j in range(4) if i or j),
        key=lambda d: -min(d[0], 4 - d[0]) - min(d[1], 4 - d[1]),
    )
    z_peers = [at_z(zmod(d), c + k - 2 * c * k) for d, k in z_order]
    pq_peers = [at_pq(pmod(i), qmod(j)) for i, j in pq_order]

    def exchange(buf, me, peers):
        k = len(used)
        for dev in peers:
            pltpu.make_async_remote_copy(
                src_ref=buf.at[me], dst_ref=buf.at[me], send_sem=xs.at[k], recv_sem=xr.at[k],
                device_id=dev, device_id_type=MESH,
            ).start()
        used.append((k, buf))

        def wait():
            some = buf.at[pl.ds(0, 15)]
            pltpu.make_async_copy(some, some, xr.at[k]).wait()

        return wait

    def joined(buf):
        peak = buf[0]
        for k in range(1, 16):
            peak = jnp.maximum(peak, buf[k])
        total = jnp.exp(buf[0] - peak)
        for k in range(1, 16):
            total = total + jnp.exp(buf[k] - peak)
        return peak + jnp.log(total)

    def in_line(v):
        return jnp.concatenate([v[j : j + 1, :] for j in range(NZ)], axis=1)

    columns_known = exchange(cstat, zc, z_peers)
    cown[...] = cstat[zc]

    def row_stats(k, carry):
        part = pl.ds(pl.multiple_of(k * 128, 128), 128)
        block = logits[part, :]
        peak = jnp.max(block, axis=1, keepdims=True)
        total = peak + jnp.log(jnp.sum(jnp.exp(block - peak), axis=1, keepdims=True))
        rvec[part, :] = 0.5 * total
        rstat[own, pl.ds(k, 1), :] = to_lanes(total)
        return carry

    lax.fori_loop(0, 4, row_stats, 0)
    rows_known = exchange(rstat, own, pq_peers)

    def start_halves(k, carry):
        part = pl.ds(pl.multiple_of(k * 128, 128), 128)
        logits[part, :] = jnp.exp(logits[part, :] - rvec[part, :] - 0.5 * in_line(cown[...]))
        return carry

    lax.fori_loop(0, 4, start_halves, 0)
    columns_known()
    cown[...] = jnp.exp(0.5 * (cown[...] - joined(cstat)))
    lane_id = lax.broadcasted_iota(jnp.int32, (1, CHUNK), 1)
    is_real = lax.rem(lane_id // PER, 2) == 1

    def masses(k, carry):
        part = pl.ds(pl.multiple_of(k * 128, 128), 128)
        total = logits[part, 0:CHUNK] * cown[0:1, :]
        for j in range(1, NZ):
            total = total + logits[part, j * CHUNK : (j + 1) * CHUNK] * cown[j : j + 1, :]
        real = jnp.sum(jnp.where(is_real, total, 0.0), axis=1, keepdims=True)
        gen = jnp.sum(jnp.where(is_real, 0.0, total), axis=1, keepdims=True)
        mstat[own, pl.ds(k, 1), :] = to_lanes(gen)
        mstat[own, pl.ds(4 + k, 1), :] = to_lanes(real)
        return carry

    lax.fori_loop(0, 4, masses, 0)
    masses_known = exchange(mstat, own, pq_peers)
    rows_known()
    joint = joined(rstat)
    shares = [jnp.exp(0.5 * (rstat[k] - joint)) for k in range(16)]
    my_share = jnp.exp(0.5 * (rstat[own] - joint))
    masses_known()
    gen = shares[0] * mstat[0, 0:4]
    real = shares[0] * mstat[0, 4:8]
    for k in range(1, 16):
        gen = gen + shares[k] * mstat[k, 0:4]
        real = real + shares[k] * mstat[k, 4:8]
    mstat[16, 0:4] = my_share * gen
    mstat[16, 4:8] = -my_share * real

    def weigh(qq, at):
        part = pl.ds(pl.multiple_of(qq * 128, 128), 128)
        on_real = to_rows(mstat[16, pl.ds(qq, 1), :])
        on_gen = to_rows(mstat[16, pl.ds(qq + 4, 1), :])
        scale = jnp.where(is_real, on_real, on_gen)
        for j in range(NZ):
            half = logits[part, j * CHUNK : (j + 1) * CHUNK] * cown[j : j + 1, :]
            weights[at, :, j * CHUNK : (j + 1) * CHUNK] = (half * scale).astype(BF16)

    def drift(w, s):
        samples = cols[:, :, :, :, s * PIECE : (s + 1) * PIECE].reshape(COLS, PIECE)
        return jnp.dot(w, samples, preferred_element_type=F32)

    before, after, across = qmod(-1), qmod(1), qmod(2)
    ahead, behind = at_pq(p, after), at_pq(p, before)
    lo, hi = pl.ds(0, 2), pl.ds(2, 2)
    weigh(across, 0)
    for s in range(SLICES):
        psend[s, 0] = drift(weights[0], s).reshape(4, PER, PIECE).astype(BF16)
        send(("f", 1, s), psend.at[s, 0, lo], far.at[s, 0], ahead)
        send(("f", -1, s), psend.at[s, 0, hi], far.at[s, 1], behind)
    weigh(after, 1)
    weigh(before, 2)
    for s in range(SLICES):
        part = drift(weights[1:3].reshape(256, COLS), s).reshape(8, PER, PIECE)
        psend[s, 1, 2:4] = part[2:4].astype(BF16)
        send(("i", 1, s), psend.at[s, 1, hi], near.at[s, 0, hi], ahead)
        psend[s, 2, 0:2] = part[4:6].astype(BF16)
        send(("i", -1, s), psend.at[s, 2, lo], near.at[s, 1, lo], behind)
        kept[s, 0:2] = part[0:2]
        kept[s, 2:4] = part[6:8]
    weigh(q, 0)
    for s in range(SLICES):
        acc[s] = drift(weights[0], s).reshape(4, PER, PIECE)
    for s in range(SLICES):
        arrived(("f", 1, s), far.at[s, 0])
        psend[s, 1, 0:2] = (kept[s, 0:2] + far[s, 0].astype(F32)).astype(BF16)
        send(("d", 1, s), psend.at[s, 1, lo], near.at[s, 0, lo], ahead)
        arrived(("f", -1, s), far.at[s, 1])
        psend[s, 2, 2:4] = (kept[s, 2:4] + far[s, 1].astype(F32)).astype(BF16)
        send(("d", -1, s), psend.at[s, 2, hi], near.at[s, 1, hi], behind)
    for s in range(SLICES):
        arrived(("i", 1, s), near.at[s, 0, hi])
        arrived(("i", -1, s), near.at[s, 1, lo])
        arrived(("d", 1, s), near.at[s, 0, lo])
        arrived(("d", -1, s), near.at[s, 1, hi])
        for d in (2, 1, 3):
            k = pmod(d)
            total = acc[s, k] + near[s, 0, k].astype(F32) + near[s, 1, k].astype(F32)
            qsend[s, d - 1] = total.astype(BF16)
            send(("r", d, s), qsend.at[s, d - 1], qrecv.at[s, d - 1], at_pq(k, q))
    square = jnp.zeros((PER, 128), F32)
    for s in range(SLICES):
        total = acc[s, p] + near[s, 0, p].astype(F32) + near[s, 1, p].astype(F32)
        for d in (1, 3, 2):
            arrived(("r", d, s), qrecv.at[s, d - 1])
            total = total + qrecv[s, d - 1].astype(F32)
        out_ref[:, s * PIECE : (s + 1) * PIECE] = total
        for k in range(PIECE // 128):
            lane = total[:, k * 128 : (k + 1) * 128]
            square = square + lane * lane
    n1[zc] = jnp.broadcast_to(jnp.sum(square, keepdims=True), (1, 128))
    first_known = exchange(n1, zc, z_peers)
    first_known()
    total = n1[0]
    for k in range(1, 16):
        total = total + n1[k]
    n2[own] = total
    second_known = exchange(n2, own, pq_peers)
    second_known()
    total = n2[0]
    for k in range(1, 16):
        total = total + n2[k]
    count = NX * NY * NZ * NC * PER * WIDTH
    out_ref[...] = out_ref[...] * lax.rsqrt(total / count + EPS)[0:1, 0:1]
    drain()


def on_device(gen, real):
    dma = pltpu.SemaphoreType.DMA
    return pl.pallas_call(
        kernel,
        out_shape=jax.ShapeDtypeStruct((PER, WIDTH), F32),
        in_specs=[pl.BlockSpec(memory_space=pl.ANY)] * 2,
        out_specs=pl.BlockSpec(memory_space=pltpu.VMEM),
        scratch_shapes=[
            pltpu.VMEM((16, PER, WIDTH), BF16),
            pltpu.VMEM((NZ, NC, 2, PER, WIDTH), BF16),
            pltpu.VMEM((ROWS, COLS), F32),
            pltpu.VMEM((ROWS, CHUNK), F32),
            pltpu.VMEM((ROWS, 1), F32),
            pltpu.VMEM((NZ, CHUNK), F32),
            pltpu.VMEM((NZ, CHUNK), F32),
            pltpu.VMEM((16, NZ, CHUNK), F32),
            pltpu.VMEM((16, 4, 128), F32),
            pltpu.VMEM((17, 8, 128), F32),
            pltpu.VMEM((16, 1, 128), F32),
            pltpu.VMEM((16, 1, 128), F32),
            pltpu.VMEM((3, 128, COLS), BF16),
            pltpu.VMEM((SLICES, 3, 4, PER, PIECE), BF16),
            pltpu.VMEM((SLICES, 4, PER, PIECE), F32),
            pltpu.VMEM((SLICES, 4, PER, PIECE), F32),
            pltpu.VMEM((SLICES, 2, 2, PER, PIECE), BF16),
            pltpu.VMEM((SLICES, 2, 4, PER, PIECE), BF16),
            pltpu.VMEM((SLICES, 3, PER, PIECE), BF16),
            pltpu.VMEM((SLICES, 3, PER, PIECE), BF16),
            dma((3,)), dma((5,)), dma((SEMS,)), dma((5,)), dma((5,)),
        ],
        compiler_params=pltpu.CompilerParams(
            collective_id=0, has_side_effects=True, vmem_limit_bytes=60 * 1024 * 1024
        ),
    )(gen, real)


def solution(mesh):
    torus = Mesh(mesh.devices.reshape(NZ, NY, NC, NX), AXES)
    return jax.shard_map(
        on_device,
        mesh=torus,
        in_specs=(P(AXES, None), P(AXES, None)),
        out_specs=P(AXES, None),
        check_vma=False,
    )
```

```python
import jax
import jax.numpy as jnp
from jax import lax
from jax.experimental import pallas as pl
from jax.experimental.pallas import tpu as pltpu
from jax.sharding import Mesh
from jax.sharding import PartitionSpec as P

AXES = ("z", "y", "c", "x")
NZ, NY, NC, NX = 8, 4, 2, 4
PER = 32
HALF = PER // 2
WIDTH = 2048
ROWS = NX * NY * PER
CHUNK = 2 * NC * PER
COLS = NZ * CHUNK
SLICES = 4
PIECE = WIDTH // SLICES
INV_SCALE = 1.0 / 0.3
MASKED = -1e30
EPS = 1e-6
F32 = jnp.float32
BF16 = jnp.bfloat16
MESH = pl.DeviceIdType.MESH
SEMS = 41


def eye():
    return lax.broadcasted_iota(jnp.int32, (128, 128), 0) == lax.broadcasted_iota(
        jnp.int32, (128, 128), 1
    )


def to_lanes(v):
    return jnp.sum(jnp.where(eye(), jnp.broadcast_to(v, (128, 128)), 0.0), axis=0, keepdims=True)


def to_rows(v):
    return jnp.sum(jnp.where(eye(), jnp.broadcast_to(v, (128, 128)), 0.0), axis=1, keepdims=True)


def kernel(
    gen_ref, real_ref, out_ref,
    rows, cols, logits, rsq, rvec, csq, cown,
    cstat, rstat, mstat, n1, n2,
    weights, psend, acc, kept, far, near, qsend, qrecv,
    in_sem, ssem, rsem, xs, xr,
):
    z, y, c, x = (lax.axis_index(a) for a in AXES)
    p = x * (1 - c) + y * c
    q = y * (1 - c) + x * c

    def at_z(zz, cc=c):
        return {"z": zz, "y": y, "c": cc, "x": x}

    def at_pq(pp, qq):
        return {"z": z, "y": qq * (1 - c) + pp * c, "c": c, "x": pp * (1 - c) + qq * c}

    def zmod(d):
        return lax.rem(z + (d + NZ), NZ)

    def pmod(d):
        return lax.rem(p + (d + 4), 4)

    def qmod(d):
        return lax.rem(q + (d + 4), 4)

    sibling = at_z(z, 1 - c)
    used, index = [], {}
    kinds = ("z", "s", "p", "f", "r")

    def drain():
        sent = (rows.at[pl.ds(0, 14)], rows, rows.at[pl.ds(0, 15)], psend, qsend)
        for k, ref in enumerate(sent):
            pltpu.make_async_copy(ref, ref, ssem.at[k]).wait()
        for k, buf in used:
            some = buf.at[pl.ds(0, 15)]
            pltpu.make_async_copy(some, some, xs.at[k]).wait()

    def send(key, src, dst, dev):
        k = index.setdefault(key, len(index))
        kind = {"q": "p", "n": "f"}.get(key[0][0], key[0][0])
        pltpu.make_async_remote_copy(
            src_ref=src, dst_ref=dst, send_sem=ssem.at[kinds.index(kind)], recv_sem=rsem.at[k],
            device_id=dev, device_id_type=MESH,
        ).start()

    def arrived(key, ref):
        pltpu.make_async_copy(ref, ref, rsem.at[index[key]]).wait()

    own = q * 4 + p
    loads = (
        pltpu.make_async_copy(gen_ref, rows.at[own], in_sem),
        pltpu.make_async_copy(gen_ref, cols.at[z, c, 0], in_sem),
        pltpu.make_async_copy(real_ref, cols.at[z, c, 1], in_sem),
    )
    for copy in loads:
        copy.start()
    barrier = pltpu.get_barrier_semaphore()
    around = (
        sibling, at_z(zmod(1)), at_z(zmod(-1)),
        at_pq(pmod(1), q), at_pq(pmod(-1), q), at_pq(p, qmod(1)), at_pq(p, qmod(-1)),
    )
    for dev in around:
        pl.semaphore_signal(barrier, inc=1, device_id=dev, device_id_type=MESH)
    pl.semaphore_wait(barrier, len(around))
    pltpu.make_async_copy(rows.at[pl.ds(0, 3)], rows.at[pl.ds(0, 3)], in_sem).wait()

    top, low = pl.ds(0, HALF), pl.ds(HALF, HALF)

    def z_piece(d, h, j):
        kind = j // 2 if d == 0 else 1 - j // 2
        return cols.at[zmod((2 * d - 1) * h), c, kind, low if j % 2 else top], kind

    def z_send(d, h, j):
        src, _ = z_piece(d, h - 1, j)
        send(("z", h, j), src, src, at_z(zmod(1 - 2 * d)))

    def z_arrive(h, j):
        arrived(("z", h, j), cols.at[0, 0, 0])
        for d in (0, 1):
            if h < 3 or (h == 3 and j < 2):
                z_send(d, h + 1, j)
        for d in (0, 1):
            src, kind = z_piece(d, h, j)
            if h == 4:
                send(("s", h), src, src, sibling)
            elif h < 4 and j % 2:
                whole = cols.at[zmod((2 * d - 1) * h), c, kind]
                send(("s", h), whole, whole, sibling)

    def sib_arrive(h):
        arrived(("s", h), {0: cols.at[0, 0], 4: cols.at[0, 0]}.get(h, cols.at[0]))

    def at_row(dq, dp):
        return qmod(dq) * 4 + pmod(dp)

    def q_sends(dp):
        block = rows.at[at_row(0, dp)]
        send(("q", dp), block, block, at_pq(p, qmod(1)))
        send(("q", dp), block, block, at_pq(p, qmod(-1)))

    def p_arrive():
        arrived(("p",), rows.at[pl.ds(0, 2)])
        for d in (1, -1):
            half = rows.at[at_row(0, -d), top if d > 0 else low]
            send(("pf",), half, half, at_pq(pmod(d), q))
        q_sends(-1)
        q_sends(1)

    def p_far():
        arrived(("pf",), rows.at[0])
        q_sends(2)

    def q_arrive(dp):
        arrived(("q", dp), rows.at[pl.ds(0, 2)])
        for d in (1, -1):
            half = rows.at[at_row(-d, dp), top if d > 0 else low]
            send(("qf", dp), half, half, at_pq(p, qmod(d)))

    def q_far(dp):
        arrived(("qf", dp), rows.at[0])

    def squares_of(value):
        value = value.astype(F32)
        return jnp.sum(value * value, axis=1, keepdims=True)

    def row_squares(dq):
        def one(k, carry):
            g = qmod(dq) * 4 + k
            rsq[pl.ds(g * PER, PER), :] = jnp.broadcast_to(squares_of(rows[g]), (PER, CHUNK))
            return carry
        lax.fori_loop(0, 4, one, 0)

    def col_squares(d):
        csq[pl.ds(zmod(d), 1), :] = to_lanes(squares_of(cols[zmod(d)].reshape(CHUNK, WIDTH)))

    def lanes_of(d):
        return pl.ds(pl.multiple_of(zmod(d) * CHUNK, CHUNK), CHUNK)

    zc = z * NC + c

    def tile(*ds):
        rhs = [cols[zmod(d)].reshape(CHUNK, WIDTH) for d in ds]
        rhs = jnp.concatenate(rhs, axis=0) if len(rhs) > 1 else rhs[0]
        inner = lax.dot_general(
            rows[...].reshape(ROWS, WIDTH), rhs, (((1,), (1,)), ((), ())),
            preferred_element_type=F32,
        )
        for k, d in enumerate(ds):
            gap = rsq[...] + csq[pl.ds(zmod(d), 1), :] - 2.0 * inner[:, k * CHUNK : (k + 1) * CHUNK]
            gap = jnp.maximum(gap, 1.0)
            logits[:, lanes_of(d)] = gap * lax.rsqrt(gap) * -INV_SCALE
        if ds == (0,):
            mine = pl.ds(pl.multiple_of(own * PER, PER), PER)
            block = logits[mine, lanes_of(0)]
            lane_id = lax.broadcasted_iota(jnp.int32, block.shape, 1)
            row_id = lax.broadcasted_iota(jnp.int32, block.shape, 0)
            logits[mine, lanes_of(0)] = jnp.where(lane_id == row_id + c * 2 * PER, MASKED, block)
        for d in ds:
            block = logits[:, lanes_of(d)]
            peak = jnp.max(block, axis=0, keepdims=True)
            total = jnp.sum(jnp.exp(block - peak), axis=0, keepdims=True)
            cstat[zc, pl.ds(zmod(d), 1), :] = peak + jnp.log(total)

    for j in range(4):
        for d in (0, 1):
            z_send(d, 1, j)
    for d in (1, -1):
        send(("p",), rows.at[own], rows.at[own], at_pq(pmod(d), q))
    q_sends(0)
    for kind in (0, 1):
        send(("s", 0), cols.at[z, c, kind], cols.at[z, c, kind], sibling)

    events = []

    def plan(when, what, *args):
        events.append((when, len(events), what, args))

    for h in range(1, 5):
        for j in range(4 if h < 4 else 2):
            plan(3.0 + 1.4 * ((h - 1) * 4 + j + 1), z_arrive, h, j)
    plan(4.8, p_arrive)
    plan(6.5, q_arrive, 0)
    plan(9.0, p_far)
    plan(10.0, q_arrive, -1)
    plan(11.0, q_arrive, 1)
    plan(11.0, q_far, 0)
    plan(13.9, q_arrive, 2)
    plan(15.0, q_far, -1)
    plan(15.0, q_far, 1)
    plan(18.6, q_far, 2)
    plan(6.6, sib_arrive, 0)
    plan(6.6, col_squares, 0)
    plan(9.1, row_squares, 0)
    plan(12.6, sib_arrive, 1)
    plan(12.6, col_squares, 1)
    plan(12.6, col_squares, -1)
    plan(15.6, row_squares, 1)
    plan(15.6, row_squares, -1)
    plan(17.1, sib_arrive, 2)
    plan(17.1, col_squares, 2)
    plan(17.1, col_squares, -2)
    plan(18.6, row_squares, 2)
    plan(18.6, tile, 0)
    plan(19.9, tile, 1, -1)
    plan(22.605, tile, 2, -2)
    plan(22.61, sib_arrive, 3)
    plan(22.62, col_squares, 3)
    plan(22.63, col_squares, -3)
    plan(22.64, tile, 3, -3)
    for _, _, what, args in sorted(events, key=lambda e: e[:2]):
        what(*args)
    sib_arrive(4)
    col_squares(4)
    tile(4)

    z_order = [(d, k) for d in (4, 3, -3, 2, -2, 1, -1, 0) for k in (1, 0) if d or k]
    pq_order = sorted(
        ((i, j) for i in range(4) for j in range(4) if i or j),
        key=lambda d: -min(d[0], 4 - d[0]) - min(d[1], 4 - d[1]),
    )
    z_peers = [at_z(zmod(d), c + k - 2 * c * k) for d, k in z_order]
    pq_peers = [at_pq(pmod(i), qmod(j)) for i, j in pq_order]

    def exchange(buf, me, peers):
        k = len(used)
        for dev in peers:
            pltpu.make_async_remote_copy(
                src_ref=buf.at[me], dst_ref=buf.at[me], send_sem=xs.at[k], recv_sem=xr.at[k],
                device_id=dev, device_id_type=MESH,
            ).start()
        used.append((k, buf))

        def wait():
            some = buf.at[pl.ds(0, 15)]
            pltpu.make_async_copy(some, some, xr.at[k]).wait()

        return wait

    def joined(buf):
        peak = buf[0]
        for k in range(1, 16):
            peak = jnp.maximum(peak, buf[k])
        total = jnp.exp(buf[0] - peak)
        for k in range(1, 16):
            total = total + jnp.exp(buf[k] - peak)
        return peak + jnp.log(total)

    def in_line(v):
        return jnp.concatenate([v[j : j + 1, :] for j in range(NZ)], axis=1)

    columns_known = exchange(cstat, zc, z_peers)
    cown[...] = cstat[zc]

    def row_stats(k, carry):
        part = pl.ds(pl.multiple_of(k * 128, 128), 128)
        block = logits[part, :]
        peak = jnp.max(block, axis=1, keepdims=True)
        total = peak + jnp.log(jnp.sum(jnp.exp(block - peak), axis=1, keepdims=True))
        rvec[part, :] = 0.5 * total
        rstat[own, pl.ds(k, 1), :] = to_lanes(total)
        return carry

    lax.fori_loop(0, 4, row_stats, 0)
    rows_known = exchange(rstat, own, pq_peers)

    def start_halves(k, carry):
        part = pl.ds(pl.multiple_of(k * 128, 128), 128)
        logits[part, :] = jnp.exp(logits[part, :] - rvec[part, :] - 0.5 * in_line(cown[...]))
        return carry

    lax.fori_loop(0, 4, start_halves, 0)
    columns_known()
    cown[...] = jnp.exp(0.5 * (cown[...] - joined(cstat)))
    lane_id = lax.broadcasted_iota(jnp.int32, (1, CHUNK), 1)
    is_real = lax.rem(lane_id // PER, 2) == 1

    def masses(k, carry):
        part = pl.ds(pl.multiple_of(k * 128, 128), 128)
        total = logits[part, 0:CHUNK] * cown[0:1, :]
        for j in range(1, NZ):
            total = total + logits[part, j * CHUNK : (j + 1) * CHUNK] * cown[j : j + 1, :]
        real = jnp.sum(jnp.where(is_real, total, 0.0), axis=1, keepdims=True)
        gen = jnp.sum(jnp.where(is_real, 0.0, total), axis=1, keepdims=True)
        mstat[own, pl.ds(k, 1), :] = to_lanes(gen)
        mstat[own, pl.ds(4 + k, 1), :] = to_lanes(real)
        return carry

    lax.fori_loop(0, 4, masses, 0)
    masses_known = exchange(mstat, own, pq_peers)
    rows_known()
    joint = joined(rstat)
    shares = [jnp.exp(0.5 * (rstat[k] - joint)) for k in range(16)]
    my_share = jnp.exp(0.5 * (rstat[own] - joint))
    masses_known()
    gen = shares[0] * mstat[0, 0:4]
    real = shares[0] * mstat[0, 4:8]
    for k in range(1, 16):
        gen = gen + shares[k] * mstat[k, 0:4]
        real = real + shares[k] * mstat[k, 4:8]
    mstat[16, 0:4] = my_share * gen
    mstat[16, 4:8] = -my_share * real

    def weigh(qq, at):
        part = pl.ds(pl.multiple_of(qq * 128, 128), 128)
        on_real = to_rows(mstat[16, pl.ds(qq, 1), :])
        on_gen = to_rows(mstat[16, pl.ds(qq + 4, 1), :])
        scale = jnp.where(is_real, on_real, on_gen)
        for j in range(NZ):
            half = logits[part, j * CHUNK : (j + 1) * CHUNK] * cown[j : j + 1, :]
            weights[at, :, j * CHUNK : (j + 1) * CHUNK] = (half * scale).astype(BF16)

    def drift(w, s):
        samples = cols[:, :, :, :, s * PIECE : (s + 1) * PIECE].reshape(COLS, PIECE)
        return jnp.dot(w, samples, preferred_element_type=F32)

    before, after, across = qmod(-1), qmod(1), qmod(2)
    ahead, behind = at_pq(p, after), at_pq(p, before)
    lo, hi = pl.ds(0, 2), pl.ds(2, 2)
    weigh(across, 0)
    for s in range(SLICES):
        psend[s, 0] = drift(weights[0], s).reshape(4, PER, PIECE).astype(BF16)
        send(("f", s), psend.at[s, 0, lo], far.at[s, 0], ahead)
        send(("f", s), psend.at[s, 0, hi], far.at[s, 1], behind)
    weigh(after, 1)
    weigh(before, 2)
    for s in range(SLICES):
        part = drift(weights[1:3].reshape(256, COLS), s).reshape(8, PER, PIECE)
        psend[s, 1, 2:4] = part[2:4].astype(BF16)
        send(("n", s), psend.at[s, 1, hi], near.at[s, 0, hi], ahead)
        psend[s, 2, 0:2] = part[4:6].astype(BF16)
        send(("n", s), psend.at[s, 2, lo], near.at[s, 1, lo], behind)
        kept[s, 0:2] = part[0:2]
        kept[s, 2:4] = part[6:8]
    weigh(q, 0)
    for s in range(SLICES):
        acc[s] = drift(weights[0], s).reshape(4, PER, PIECE)
    for s in range(SLICES):
        arrived(("f", s), far.at[s])
        psend[s, 1, 0:2] = (kept[s, 0:2] + far[s, 0].astype(F32)).astype(BF16)
        send(("n", s), psend.at[s, 1, lo], near.at[s, 0, lo], ahead)
        psend[s, 2, 2:4] = (kept[s, 2:4] + far[s, 1].astype(F32)).astype(BF16)
        send(("n", s), psend.at[s, 2, hi], near.at[s, 1, hi], behind)
    for s in range(SLICES):
        arrived(("n", s), near.at[s])
        for d in (2, 1, 3):
            k = pmod(d)
            total = acc[s, k] + near[s, 0, k].astype(F32) + near[s, 1, k].astype(F32)
            qsend[s, d - 1] = total.astype(BF16)
            send(("r", s), qsend.at[s, d - 1], qrecv.at[s, d - 1], at_pq(k, q))
    square = jnp.zeros((PER, 128), F32)
    for s in range(SLICES):
        total = acc[s, p] + near[s, 0, p].astype(F32) + near[s, 1, p].astype(F32)
        arrived(("r", s), qrecv.at[s])
        for d in (1, 3, 2):
            total = total + qrecv[s, d - 1].astype(F32)
        out_ref[:, s * PIECE : (s + 1) * PIECE] = total
        for k in range(PIECE // 128):
            lane = total[:, k * 128 : (k + 1) * 128]
            square = square + lane * lane
    n1[zc] = jnp.broadcast_to(jnp.sum(square, keepdims=True), (1, 128))
    first_known = exchange(n1, zc, z_peers)
    first_known()
    total = n1[0]
    for k in range(1, 16):
        total = total + n1[k]
    n2[own] = total
    second_known = exchange(n2, own, pq_peers)
    second_known()
    total = n2[0]
    for k in range(1, 16):
        total = total + n2[k]
    count = NX * NY * NZ * NC * PER * WIDTH
    out_ref[...] = out_ref[...] * lax.rsqrt(total / count + EPS)[0:1, 0:1]
    drain()


def on_device(gen, real):
    dma = pltpu.SemaphoreType.DMA
    return pl.pallas_call(
        kernel,
        out_shape=jax.ShapeDtypeStruct((PER, WIDTH), F32),
        in_specs=[pl.BlockSpec(memory_space=pl.ANY)] * 2,
        out_specs=pl.BlockSpec(memory_space=pltpu.VMEM),
        scratch_shapes=[
            pltpu.VMEM((16, PER, WIDTH), BF16),
            pltpu.VMEM((NZ, NC, 2, PER, WIDTH), BF16),
            pltpu.VMEM((ROWS, COLS), F32),
            pltpu.VMEM((ROWS, CHUNK), F32),
            pltpu.VMEM((ROWS, 1), F32),
            pltpu.VMEM((NZ, CHUNK), F32),
            pltpu.VMEM((NZ, CHUNK), F32),
            pltpu.VMEM((16, NZ, CHUNK), F32),
            pltpu.VMEM((16, 4, 128), F32),
            pltpu.VMEM((17, 8, 128), F32),
            pltpu.VMEM((16, 1, 128), F32),
            pltpu.VMEM((16, 1, 128), F32),
            pltpu.VMEM((3, 128, COLS), BF16),
            pltpu.VMEM((SLICES, 3, 4, PER, PIECE), BF16),
            pltpu.VMEM((SLICES, 4, PER, PIECE), F32),
            pltpu.VMEM((SLICES, 4, PER, PIECE), F32),
            pltpu.VMEM((SLICES, 2, 2, PER, PIECE), BF16),
            pltpu.VMEM((SLICES, 2, 4, PER, PIECE), BF16),
            pltpu.VMEM((SLICES, 3, PER, PIECE), BF16),
            pltpu.VMEM((SLICES, 3, PER, PIECE), BF16),
            dma, dma((5,)), dma((SEMS,)), dma((5,)), dma((5,)),
        ],
        compiler_params=pltpu.CompilerParams(
            collective_id=0, has_side_effects=True, vmem_limit_bytes=60 * 1024 * 1024
        ),
    )(gen, real)


def solution(mesh):
    torus = Mesh(mesh.devices.reshape(NZ, NY, NC, NX), AXES)
    return jax.shard_map(
        on_device,
        mesh=torus,
        in_specs=(P(AXES, None), P(AXES, None)),
        out_specs=P(AXES, None),
        check_vma=False,
    )
```

```python
import jax
import jax.numpy as jnp
from jax import lax
from jax.experimental import pallas as pl
from jax.experimental.pallas import tpu as pltpu
from jax.sharding import Mesh
from jax.sharding import PartitionSpec as P

AXES = ("z", "y", "c", "x")
NZ, NY, NC, NX = 8, 4, 2, 4
PER = 32
HALF = PER // 2
WIDTH = 2048
ROWS = NX * NY * PER
CHUNK = 2 * NC * PER
COLS = NZ * CHUNK
SLICES = 4
PIECE = WIDTH // SLICES
INV_SCALE = 1.0 / 0.3
MASKED = -1e30
EPS = 1e-6
F32 = jnp.float32
BF16 = jnp.bfloat16
MESH = pl.DeviceIdType.MESH
SEMS = 44


def eye():
    return lax.broadcasted_iota(jnp.int32, (128, 128), 0) == lax.broadcasted_iota(
        jnp.int32, (128, 128), 1
    )


def to_lanes(v):
    return jnp.sum(jnp.where(eye(), jnp.broadcast_to(v, (128, 128)), 0.0), axis=0, keepdims=True)


def to_rows(v):
    return jnp.sum(jnp.where(eye(), jnp.broadcast_to(v, (128, 128)), 0.0), axis=1, keepdims=True)


def kernel(
    gen_ref, real_ref, out_ref,
    rows, cols, logits, rsq, rvec, csq, cown,
    cstat, rstat, mstat, n1, n2,
    weights, psend, acc, kept, far, near, qsend, qrecv, relay,
    in_sem, ssem, rsem, xs, xr,
):
    z, y, c, x = (lax.axis_index(a) for a in AXES)
    p = x * (1 - c) + y * c
    q = y * (1 - c) + x * c

    def at_z(zz, cc=c):
        return {"z": zz, "y": y, "c": cc, "x": x}

    def at_pq(pp, qq):
        return {"z": z, "y": qq * (1 - c) + pp * c, "c": c, "x": pp * (1 - c) + qq * c}

    def zmod(d):
        return lax.rem(z + (d + NZ), NZ)

    def pmod(d):
        return lax.rem(p + (d + 4), 4)

    def qmod(d):
        return lax.rem(q + (d + 4), 4)

    sibling = at_z(z, 1 - c)
    used, index = [], {}
    kinds = ("z", "s", "p", "f", "r")

    def drain():
        sent = (rows.at[pl.ds(0, 14)], rows, rows.at[pl.ds(0, 15)], psend, qsend)
        for k, ref in enumerate(sent):
            pltpu.make_async_copy(ref, ref, ssem.at[k]).wait()
        for k, buf in used:
            some = buf.at[pl.ds(0, 15)]
            pltpu.make_async_copy(some, some, xs.at[k]).wait()

    def send(key, src, dst, dev):
        k = index.setdefault(key, len(index))
        kind = {"q": "p", "n": "f", "g": "r"}.get(key[0][0], key[0][0])
        pltpu.make_async_remote_copy(
            src_ref=src, dst_ref=dst, send_sem=ssem.at[kinds.index(kind)], recv_sem=rsem.at[k],
            device_id=dev, device_id_type=MESH,
        ).start()

    def arrived(key, ref):
        pltpu.make_async_copy(ref, ref, rsem.at[index[key]]).wait()

    own = q * 4 + p
    loads = (
        pltpu.make_async_copy(gen_ref, rows.at[own], in_sem),
        pltpu.make_async_copy(gen_ref, cols.at[z, c, 0], in_sem),
        pltpu.make_async_copy(real_ref, cols.at[z, c, 1], in_sem),
    )
    for copy in loads:
        copy.start()
    barrier = pltpu.get_barrier_semaphore()
    around = (
        sibling, at_z(zmod(1)), at_z(zmod(-1)),
        at_pq(pmod(1), q), at_pq(pmod(-1), q), at_pq(p, qmod(1)), at_pq(p, qmod(-1)),
    )
    for dev in around:
        pl.semaphore_signal(barrier, inc=1, device_id=dev, device_id_type=MESH)
    pl.semaphore_wait(barrier, len(around))
    pltpu.make_async_copy(rows.at[pl.ds(0, 3)], rows.at[pl.ds(0, 3)], in_sem).wait()

    top, low = pl.ds(0, HALF), pl.ds(HALF, HALF)

    def z_piece(d, h, j):
        kind = j // 2 if d == 0 else 1 - j // 2
        return cols.at[zmod((2 * d - 1) * h), c, kind, low if j % 2 else top], kind

    def z_send(d, h, j):
        src, _ = z_piece(d, h - 1, j)
        send(("z", h, j), src, src, at_z(zmod(1 - 2 * d)))

    def z_arrive(h, j):
        arrived(("z", h, j), cols.at[0, 0, 0])
        for d in (0, 1):
            if h < 3 or (h == 3 and j < 2):
                z_send(d, h + 1, j)
        for d in (0, 1):
            src, kind = z_piece(d, h, j)
            if h == 4:
                send(("s", h), src, src, sibling)
            elif h < 4 and j % 2:
                whole = cols.at[zmod((2 * d - 1) * h), c, kind]
                send(("s", h), whole, whole, sibling)

    def sib_arrive(h):
        arrived(("s", h), {0: cols.at[0, 0], 4: cols.at[0, 0]}.get(h, cols.at[0]))

    def at_row(dq, dp):
        return qmod(dq) * 4 + pmod(dp)

    def q_sends(dp):
        block = rows.at[at_row(0, dp)]
        send(("q", dp), block, block, at_pq(p, qmod(1)))
        send(("q", dp), block, block, at_pq(p, qmod(-1)))

    def p_arrive():
        arrived(("p",), rows.at[pl.ds(0, 2)])
        for d in (1, -1):
            half = rows.at[at_row(0, -d), top if d > 0 else low]
            send(("pf",), half, half, at_pq(pmod(d), q))
        q_sends(-1)
        q_sends(1)

    def p_far():
        arrived(("pf",), rows.at[0])
        q_sends(2)

    def q_arrive(dp):
        arrived(("q", dp), rows.at[pl.ds(0, 2)])
        for d in (1, -1):
            half = rows.at[at_row(-d, dp), top if d > 0 else low]
            send(("qf", dp), half, half, at_pq(p, qmod(d)))

    def q_far(dp):
        arrived(("qf", dp), rows.at[0])

    def squares_of(value):
        value = value.astype(F32)
        return jnp.sum(value * value, axis=1, keepdims=True)

    def row_squares(dq):
        def one(k, carry):
            g = qmod(dq) * 4 + k
            rsq[pl.ds(g * PER, PER), :] = jnp.broadcast_to(squares_of(rows[g]), (PER, CHUNK))
            return carry
        lax.fori_loop(0, 4, one, 0)

    def col_squares(d):
        csq[pl.ds(zmod(d), 1), :] = to_lanes(squares_of(cols[zmod(d)].reshape(CHUNK, WIDTH)))

    def lanes_of(d):
        return pl.ds(pl.multiple_of(zmod(d) * CHUNK, CHUNK), CHUNK)

    zc = z * NC + c

    def tile(*ds):
        rhs = [cols[zmod(d)].reshape(CHUNK, WIDTH) for d in ds]
        rhs = jnp.concatenate(rhs, axis=0) if len(rhs) > 1 else rhs[0]
        inner = lax.dot_general(
            rows[...].reshape(ROWS, WIDTH), rhs, (((1,), (1,)), ((), ())),
            preferred_element_type=F32,
        )
        for k, d in enumerate(ds):
            gap = rsq[...] + csq[pl.ds(zmod(d), 1), :] - 2.0 * inner[:, k * CHUNK : (k + 1) * CHUNK]
            gap = jnp.maximum(gap, 1.0)
            logits[:, lanes_of(d)] = gap * lax.rsqrt(gap) * -INV_SCALE
        if ds == (0,):
            mine = pl.ds(pl.multiple_of(own * PER, PER), PER)
            block = logits[mine, lanes_of(0)]
            lane_id = lax.broadcasted_iota(jnp.int32, block.shape, 1)
            row_id = lax.broadcasted_iota(jnp.int32, block.shape, 0)
            logits[mine, lanes_of(0)] = jnp.where(lane_id == row_id + c * 2 * PER, MASKED, block)
        for d in ds:
            block = logits[:, lanes_of(d)]
            peak = jnp.max(block, axis=0, keepdims=True)
            total = jnp.sum(jnp.exp(block - peak), axis=0, keepdims=True)
            cstat[zc, pl.ds(zmod(d), 1), :] = peak + jnp.log(total)

    for j in range(4):
        for d in (0, 1):
            z_send(d, 1, j)
    for d in (1, -1):
        send(("p",), rows.at[own], rows.at[own], at_pq(pmod(d), q))
    q_sends(0)
    for kind in (0, 1):
        send(("s", 0), cols.at[z, c, kind], cols.at[z, c, kind], sibling)

    events = []

    def plan(when, what, *args):
        events.append((when, len(events), what, args))

    for h in range(1, 5):
        for j in range(4 if h < 4 else 2):
            plan(3.0 + 1.4 * ((h - 1) * 4 + j + 1), z_arrive, h, j)
    plan(4.8, p_arrive)
    plan(6.5, q_arrive, 0)
    plan(9.0, p_far)
    plan(10.0, q_arrive, -1)
    plan(11.0, q_arrive, 1)
    plan(11.0, q_far, 0)
    plan(13.9, q_arrive, 2)
    plan(15.0, q_far, -1)
    plan(15.0, q_far, 1)
    plan(18.6, q_far, 2)
    plan(6.6, sib_arrive, 0)
    plan(6.6, col_squares, 0)
    plan(9.1, row_squares, 0)
    plan(12.6, sib_arrive, 1)
    plan(12.6, col_squares, 1)
    plan(12.6, col_squares, -1)
    plan(15.6, row_squares, 1)
    plan(15.6, row_squares, -1)
    plan(17.1, sib_arrive, 2)
    plan(17.1, col_squares, 2)
    plan(17.1, col_squares, -2)
    plan(18.6, row_squares, 2)
    plan(18.6, tile, 0)
    plan(19.9, tile, 1, -1)
    plan(22.605, tile, 2, -2)
    plan(22.61, sib_arrive, 3)
    plan(22.62, col_squares, 3)
    plan(22.63, col_squares, -3)
    plan(22.64, tile, 3, -3)
    for _, _, what, args in sorted(events, key=lambda e: e[:2]):
        what(*args)
    sib_arrive(4)
    col_squares(4)
    tile(4)

    z_order = [(d, k) for d in (4, 3, -3, 2, -2, 1, -1, 0) for k in (1, 0) if d or k]
    pq_order = sorted(
        ((i, j) for i in range(4) for j in range(4) if i or j),
        key=lambda d: -min(d[0], 4 - d[0]) - min(d[1], 4 - d[1]),
    )
    z_peers = [at_z(zmod(d), c + k - 2 * c * k) for d, k in z_order]
    pq_peers = [at_pq(pmod(i), qmod(j)) for i, j in pq_order]

    def exchange(buf, me, peers):
        k = len(used)
        for dev in peers:
            pltpu.make_async_remote_copy(
                src_ref=buf.at[me], dst_ref=buf.at[me], send_sem=xs.at[k], recv_sem=xr.at[k],
                device_id=dev, device_id_type=MESH,
            ).start()
        used.append((k, buf))

        def wait():
            some = buf.at[pl.ds(0, 15)]
            pltpu.make_async_copy(some, some, xr.at[k]).wait()

        return wait

    def joined(buf):
        peak = buf[0]
        for k in range(1, 16):
            peak = jnp.maximum(peak, buf[k])
        total = jnp.exp(buf[0] - peak)
        for k in range(1, 16):
            total = total + jnp.exp(buf[k] - peak)
        return peak + jnp.log(total)

    def in_line(v):
        return jnp.concatenate([v[j : j + 1, :] for j in range(NZ)], axis=1)

    columns_known = exchange(cstat, zc, z_peers)
    cown[...] = cstat[zc]

    def row_stats(k, carry):
        part = pl.ds(pl.multiple_of(k * 128, 128), 128)
        block = logits[part, :]
        peak = jnp.max(block, axis=1, keepdims=True)
        total = peak + jnp.log(jnp.sum(jnp.exp(block - peak), axis=1, keepdims=True))
        rvec[part, :] = 0.5 * total
        rstat[own, pl.ds(k, 1), :] = to_lanes(total)
        return carry

    lax.fori_loop(0, 4, row_stats, 0)
    rows_known = exchange(rstat, own, pq_peers)

    def start_halves(k, carry):
        part = pl.ds(pl.multiple_of(k * 128, 128), 128)
        logits[part, :] = jnp.exp(logits[part, :] - rvec[part, :] - 0.5 * in_line(cown[...]))
        return carry

    lax.fori_loop(0, 4, start_halves, 0)
    columns_known()
    cown[...] = jnp.exp(0.5 * (cown[...] - joined(cstat)))
    lane_id = lax.broadcasted_iota(jnp.int32, (1, CHUNK), 1)
    is_real = lax.rem(lane_id // PER, 2) == 1

    def masses(k, carry):
        part = pl.ds(pl.multiple_of(k * 128, 128), 128)
        total = logits[part, 0:CHUNK] * cown[0:1, :]
        for j in range(1, NZ):
            total = total + logits[part, j * CHUNK : (j + 1) * CHUNK] * cown[j : j + 1, :]
        real = jnp.sum(jnp.where(is_real, total, 0.0), axis=1, keepdims=True)
        gen = jnp.sum(jnp.where(is_real, 0.0, total), axis=1, keepdims=True)
        mstat[own, pl.ds(k, 1), :] = to_lanes(gen)
        mstat[own, pl.ds(4 + k, 1), :] = to_lanes(real)
        return carry

    lax.fori_loop(0, 4, masses, 0)
    masses_known = exchange(mstat, own, pq_peers)
    rows_known()
    joint = joined(rstat)
    shares = [jnp.exp(0.5 * (rstat[k] - joint)) for k in range(16)]
    my_share = jnp.exp(0.5 * (rstat[own] - joint))
    masses_known()
    gen = shares[0] * mstat[0, 0:4]
    real = shares[0] * mstat[0, 4:8]
    for k in range(1, 16):
        gen = gen + shares[k] * mstat[k, 0:4]
        real = real + shares[k] * mstat[k, 4:8]
    mstat[16, 0:4] = my_share * gen
    mstat[16, 4:8] = -my_share * real

    def weigh(qq, at):
        part = pl.ds(pl.multiple_of(qq * 128, 128), 128)
        on_real = to_rows(mstat[16, pl.ds(qq, 1), :])
        on_gen = to_rows(mstat[16, pl.ds(qq + 4, 1), :])
        scale = jnp.where(is_real, on_real, on_gen)
        for j in range(NZ):
            half = logits[part, j * CHUNK : (j + 1) * CHUNK] * cown[j : j + 1, :]
            weights[at, :, j * CHUNK : (j + 1) * CHUNK] = (half * scale).astype(BF16)

    def drift(w, s):
        samples = cols[:, :, :, :, s * PIECE : (s + 1) * PIECE].reshape(COLS, PIECE)
        return jnp.dot(w, samples, preferred_element_type=F32)

    before, after, across = qmod(-1), qmod(1), qmod(2)
    ahead, behind = at_pq(p, after), at_pq(p, before)
    p_ahead, p_behind = at_pq(pmod(1), q), at_pq(pmod(-1), q)
    lo, hi = pl.ds(0, 2), pl.ds(2, 2)
    weigh(across, 0)
    for s in range(SLICES):
        psend[s, 0] = drift(weights[0], s).reshape(4, PER, PIECE).astype(BF16)
        send(("f", s), psend.at[s, 0, lo], far.at[s, 0], ahead)
        send(("f", s), psend.at[s, 0, hi], far.at[s, 1], behind)
    weigh(after, 1)
    weigh(before, 2)
    for s in range(SLICES):
        part = drift(weights[1:3].reshape(256, COLS), s).reshape(8, PER, PIECE)
        psend[s, 1, 2:4] = part[2:4].astype(BF16)
        send(("n", s), psend.at[s, 1, hi], near.at[s, 0, hi], ahead)
        psend[s, 2, 0:2] = part[4:6].astype(BF16)
        send(("n", s), psend.at[s, 2, lo], near.at[s, 1, lo], behind)
        kept[s, 0:2] = part[0:2]
        kept[s, 2:4] = part[6:8]
    weigh(q, 0)
    for s in range(SLICES):
        acc[s] = drift(weights[0], s).reshape(4, PER, PIECE)
    for s in range(SLICES):
        arrived(("f", s), far.at[s])
        psend[s, 1, 0:2] = (kept[s, 0:2] + far[s, 0].astype(F32)).astype(BF16)
        send(("n", s), psend.at[s, 1, lo], near.at[s, 0, lo], ahead)
        psend[s, 2, 2:4] = (kept[s, 2:4] + far[s, 1].astype(F32)).astype(BF16)
        send(("n", s), psend.at[s, 2, hi], near.at[s, 1, hi], behind)
    for s in range(SLICES):
        arrived(("n", s), near.at[s])
        share = [
            acc[s, pmod(d)] + near[s, 0, pmod(d)].astype(F32) + near[s, 1, pmod(d)].astype(F32)
            for d in (1, 2, 3)
        ]
        if s == SLICES - 1:
            for d in (2, 1, 3):
                qsend[s, d - 1] = share[d - 1].astype(BF16)
                send(("r", s), qsend.at[s, d - 1], qrecv.at[s, d - 1], at_pq(pmod(d), q))
            continue
        qsend[s, 1] = share[1].astype(BF16)
        send(("g", s), qsend.at[s, 1, top], relay.at[s, 0], p_ahead)
        send(("g", s), qsend.at[s, 1, low], relay.at[s, 1], p_behind)
        qsend[s, 0, HALF:] = share[0][HALF:].astype(BF16)
        send(("r", s), qsend.at[s, 0, low], qrecv.at[s, 0, low], p_ahead)
        qsend[s, 2, :HALF] = share[2][:HALF].astype(BF16)
        send(("r", s), qsend.at[s, 2, top], qrecv.at[s, 2, top], p_behind)
        acc[s, pmod(1), :HALF] = share[0][:HALF]
        acc[s, pmod(3), HALF:] = share[2][HALF:]
    for s in range(SLICES - 1):
        arrived(("g", s), relay.at[s])
        qsend[s, 0, :HALF] = (acc[s, pmod(1), :HALF] + relay[s, 0].astype(F32)).astype(BF16)
        send(("r", s), qsend.at[s, 0, top], qrecv.at[s, 0, top], p_ahead)
        qsend[s, 2, HALF:] = (acc[s, pmod(3), HALF:] + relay[s, 1].astype(F32)).astype(BF16)
        send(("r", s), qsend.at[s, 2, low], qrecv.at[s, 2, low], p_behind)
    square = jnp.zeros((PER, 128), F32)
    for s in range(SLICES):
        total = acc[s, p] + near[s, 0, p].astype(F32) + near[s, 1, p].astype(F32)
        direct = s == SLICES - 1
        arrived(("r", s), qrecv.at[s] if direct else qrecv.at[s, pl.ds(0, 2)])
        for d in (1, 3, 2) if direct else (1, 3):
            total = total + qrecv[s, d - 1].astype(F32)
        out_ref[:, s * PIECE : (s + 1) * PIECE] = total
        for k in range(PIECE // 128):
            lane = total[:, k * 128 : (k + 1) * 128]
            square = square + lane * lane
    n1[zc] = jnp.broadcast_to(jnp.sum(square, keepdims=True), (1, 128))
    first_known = exchange(n1, zc, z_peers)
    first_known()
    total = n1[0]
    for k in range(1, 16):
        total = total + n1[k]
    n2[own] = total
    second_known = exchange(n2, own, pq_peers)
    second_known()
    total = n2[0]
    for k in range(1, 16):
        total = total + n2[k]
    count = NX * NY * NZ * NC * PER * WIDTH
    out_ref[...] = out_ref[...] * lax.rsqrt(total / count + EPS)[0:1, 0:1]
    drain()


def on_device(gen, real):
    dma = pltpu.SemaphoreType.DMA
    return pl.pallas_call(
        kernel,
        out_shape=jax.ShapeDtypeStruct((PER, WIDTH), F32),
        in_specs=[pl.BlockSpec(memory_space=pl.ANY)] * 2,
        out_specs=pl.BlockSpec(memory_space=pltpu.VMEM),
        scratch_shapes=[
            pltpu.VMEM((16, PER, WIDTH), BF16),
            pltpu.VMEM((NZ, NC, 2, PER, WIDTH), BF16),
            pltpu.VMEM((ROWS, COLS), F32),
            pltpu.VMEM((ROWS, CHUNK), F32),
            pltpu.VMEM((ROWS, 1), F32),
            pltpu.VMEM((NZ, CHUNK), F32),
            pltpu.VMEM((NZ, CHUNK), F32),
            pltpu.VMEM((16, NZ, CHUNK), F32),
            pltpu.VMEM((16, 4, 128), F32),
            pltpu.VMEM((17, 8, 128), F32),
            pltpu.VMEM((16, 1, 128), F32),
            pltpu.VMEM((16, 1, 128), F32),
            pltpu.VMEM((3, 128, COLS), BF16),
            pltpu.VMEM((SLICES, 3, 4, PER, PIECE), BF16),
            pltpu.VMEM((SLICES, 4, PER, PIECE), F32),
            pltpu.VMEM((SLICES, 4, PER, PIECE), F32),
            pltpu.VMEM((SLICES, 2, 2, PER, PIECE), BF16),
            pltpu.VMEM((SLICES, 2, 4, PER, PIECE), BF16),
            pltpu.VMEM((SLICES, 3, PER, PIECE), BF16),
            pltpu.VMEM((SLICES, 3, PER, PIECE), BF16),
            pltpu.VMEM((SLICES - 1, 2, HALF, PIECE), BF16),
            dma, dma((5,)), dma((SEMS,)), dma((5,)), dma((5,)),
        ],
        compiler_params=pltpu.CompilerParams(
            collective_id=0, has_side_effects=True, vmem_limit_bytes=60 * 1024 * 1024
        ),
    )(gen, real)


def solution(mesh):
    torus = Mesh(mesh.devices.reshape(NZ, NY, NC, NX), AXES)
    return jax.shard_map(
        on_device,
        mesh=torus,
        in_specs=(P(AXES, None), P(AXES, None)),
        out_specs=P(AXES, None),
        check_vma=False,
    )
```

```python
import jax
import jax.numpy as jnp
from jax import lax
from jax.experimental import pallas as pl
from jax.experimental.pallas import tpu as pltpu
from jax.sharding import Mesh
from jax.sharding import PartitionSpec as P

AXES = ("z", "y", "c", "x")
NZ, NY, NC, NX = 8, 4, 2, 4
PER = 32
HALF = PER // 2
WIDTH = 2048
ROWS = NX * NY * PER
CHUNK = 2 * NC * PER
COLS = NZ * CHUNK
SLICES = 2
PIECE = WIDTH // SLICES
INV_SCALE = 1.0 / 0.3
MASKED = -1e30
EPS = 1e-6
F32 = jnp.float32
BF16 = jnp.bfloat16
MESH = pl.DeviceIdType.MESH
SEMS = 35


def eye():
    return lax.broadcasted_iota(jnp.int32, (128, 128), 0) == lax.broadcasted_iota(
        jnp.int32, (128, 128), 1
    )


def to_lanes(v):
    return jnp.sum(jnp.where(eye(), jnp.broadcast_to(v, (128, 128)), 0.0), axis=0, keepdims=True)


def to_rows(v):
    return jnp.sum(jnp.where(eye(), jnp.broadcast_to(v, (128, 128)), 0.0), axis=1, keepdims=True)


def kernel(
    gen_ref, real_ref, out_ref,
    rows, cols, logits, rsq, rvec, csq, cown,
    cstat, rstat, mstat, n1, n2,
    weights, psend, acc, kept, far, near, qsend, qrecv,
    in_sem, ssem, rsem, xs, xr,
):
    z, y, c, x = (lax.axis_index(a) for a in AXES)
    p = x * (1 - c) + y * c
    q = y * (1 - c) + x * c

    def at_z(zz, cc=c):
        return {"z": zz, "y": y, "c": cc, "x": x}

    def at_pq(pp, qq):
        return {"z": z, "y": qq * (1 - c) + pp * c, "c": c, "x": pp * (1 - c) + qq * c}

    def zmod(d):
        return lax.rem(z + (d + NZ), NZ)

    def pmod(d):
        return lax.rem(p + (d + 4), 4)

    def qmod(d):
        return lax.rem(q + (d + 4), 4)

    sibling = at_z(z, 1 - c)
    used, index = [], {}
    kinds = ("z", "s", "p", "f", "r")

    def drain():
        sent = (rows.at[pl.ds(0, 14)], rows, rows.at[pl.ds(0, 15)], psend, qsend)
        for k, ref in enumerate(sent):
            pltpu.make_async_copy(ref, ref, ssem.at[k]).wait()
        for k, buf in used:
            some = buf.at[pl.ds(0, 15)]
            pltpu.make_async_copy(some, some, xs.at[k]).wait()

    def post(k, kind, src, dst, dev):
        pltpu.make_async_remote_copy(
            src_ref=src, dst_ref=dst, send_sem=ssem.at[kinds.index(kind)], recv_sem=rsem.at[k],
            device_id=dev, device_id_type=MESH,
        ).start()

    def send(key, src, dst, dev):
        k = index.setdefault(key, len(index))
        post(k, {"q": "p"}.get(key[0][0], key[0][0]), src, dst, dev)

    def arrived(key, ref):
        pltpu.make_async_copy(ref, ref, rsem.at[index[key]]).wait()

    own = q * 4 + p
    loads = (
        pltpu.make_async_copy(gen_ref, rows.at[own], in_sem),
        pltpu.make_async_copy(gen_ref, cols.at[z, c, 0], in_sem),
        pltpu.make_async_copy(real_ref, cols.at[z, c, 1], in_sem),
    )
    for copy in loads:
        copy.start()
    barrier = pltpu.get_barrier_semaphore()
    around = (
        sibling, at_z(zmod(1)), at_z(zmod(-1)),
        at_pq(pmod(1), q), at_pq(pmod(-1), q), at_pq(p, qmod(1)), at_pq(p, qmod(-1)),
    )
    for dev in around:
        pl.semaphore_signal(barrier, inc=1, device_id=dev, device_id_type=MESH)
    pl.semaphore_wait(barrier, len(around))
    pltpu.make_async_copy(rows.at[pl.ds(0, 3)], rows.at[pl.ds(0, 3)], in_sem).wait()

    top, low = pl.ds(0, HALF), pl.ds(HALF, HALF)

    def z_piece(d, h, j):
        kind = j // 2 if d == 0 else 1 - j // 2
        return cols.at[zmod((2 * d - 1) * h), c, kind, low if j % 2 else top], kind

    def z_send(d, h, j):
        src, _ = z_piece(d, h - 1, j)
        send(("z", h, j), src, src, at_z(zmod(1 - 2 * d)))

    def z_arrive(h, j):
        arrived(("z", h, j), cols.at[0, 0, 0])
        for d in (0, 1):
            if h < 3 or (h == 3 and j < 2):
                z_send(d, h + 1, j)
        for d in (0, 1):
            src, kind = z_piece(d, h, j)
            if h == 4:
                send(("s", h), src, src, sibling)
            elif h < 4 and j % 2:
                whole = cols.at[zmod((2 * d - 1) * h), c, kind]
                send(("s", h), whole, whole, sibling)

    def sib_arrive(h):
        arrived(("s", h), {0: cols.at[0, 0], 4: cols.at[0, 0]}.get(h, cols.at[0]))

    def at_row(dq, dp):
        return qmod(dq) * 4 + pmod(dp)

    def q_sends(dp):
        block = rows.at[at_row(0, dp)]
        send(("q", dp), block, block, at_pq(p, qmod(1)))
        send(("q", dp), block, block, at_pq(p, qmod(-1)))

    def p_arrive():
        arrived(("p",), rows.at[pl.ds(0, 2)])
        for d in (1, -1):
            half = rows.at[at_row(0, -d), top if d > 0 else low]
            send(("pf",), half, half, at_pq(pmod(d), q))
        q_sends(-1)
        q_sends(1)

    def p_far():
        arrived(("pf",), rows.at[0])
        q_sends(2)

    def q_arrive(dp):
        arrived(("q", dp), rows.at[pl.ds(0, 2)])
        for d in (1, -1):
            half = rows.at[at_row(-d, dp), top if d > 0 else low]
            send(("qf", dp), half, half, at_pq(p, qmod(d)))

    def q_far(dp):
        arrived(("qf", dp), rows.at[0])

    def squares_of(value):
        value = value.astype(F32)
        return jnp.sum(value * value, axis=1, keepdims=True)

    def row_squares(dq):
        def one(k, carry):
            g = qmod(dq) * 4 + k
            rsq[pl.ds(g * PER, PER), :] = jnp.broadcast_to(squares_of(rows[g]), (PER, CHUNK))
            return carry
        lax.fori_loop(0, 4, one, 0)

    def col_squares(d):
        csq[pl.ds(zmod(d), 1), :] = to_lanes(squares_of(cols[zmod(d)].reshape(CHUNK, WIDTH)))

    def lanes_of(d):
        return pl.ds(pl.multiple_of(zmod(d) * CHUNK, CHUNK), CHUNK)

    zc = z * NC + c

    def tile(*ds):
        def rhs():
            parts = [cols[zmod(d)].reshape(CHUNK, WIDTH) for d in ds]
            return jnp.concatenate(parts, axis=0) if len(parts) > 1 else parts[0]

        block_rows = ROWS // 2

        def some_rows(b, carry):
            part = pl.ds(pl.multiple_of(b * block_rows, block_rows), block_rows)
            lhs = rows[pl.ds(b * 8, 8)].reshape(block_rows, WIDTH)
            inner = lax.dot_general(
                lhs, rhs(), (((1,), (1,)), ((), ())), preferred_element_type=F32
            )
            for k, d in enumerate(ds):
                gap = rsq[part, :] + csq[pl.ds(zmod(d), 1), :]
                gap = jnp.maximum(gap - 2.0 * inner[:, k * CHUNK : (k + 1) * CHUNK], 1.0)
                logits[part, lanes_of(d)] = gap * lax.rsqrt(gap) * -INV_SCALE
            return carry

        lax.fori_loop(0, 2, some_rows, 0)
        if ds == (0,):
            mine = pl.ds(pl.multiple_of(own * PER, PER), PER)
            block = logits[mine, lanes_of(0)]
            lane_id = lax.broadcasted_iota(jnp.int32, block.shape, 1)
            row_id = lax.broadcasted_iota(jnp.int32, block.shape, 0)
            logits[mine, lanes_of(0)] = jnp.where(lane_id == row_id + c * 2 * PER, MASKED, block)
        for d in ds:
            block = logits[:, lanes_of(d)]
            peak = jnp.max(block, axis=0, keepdims=True)
            total = jnp.sum(jnp.exp(block - peak), axis=0, keepdims=True)
            cstat[zc, pl.ds(zmod(d), 1), :] = peak + jnp.log(total)

    for j in range(4):
        for d in (0, 1):
            z_send(d, 1, j)
    for d in (1, -1):
        send(("p",), rows.at[own], rows.at[own], at_pq(pmod(d), q))
    q_sends(0)
    for kind in (0, 1):
        send(("s", 0), cols.at[z, c, kind], cols.at[z, c, kind], sibling)

    events = []

    def plan(when, what, *args):
        events.append((when, len(events), what, args))

    for h in range(1, 5):
        for j in range(4 if h < 4 else 2):
            plan(3.0 + 1.4 * ((h - 1) * 4 + j + 1), z_arrive, h, j)
    plan(4.8, p_arrive)
    plan(6.5, q_arrive, 0)
    plan(9.0, p_far)
    plan(10.0, q_arrive, -1)
    plan(11.0, q_arrive, 1)
    plan(11.0, q_far, 0)
    plan(13.9, q_arrive, 2)
    plan(15.0, q_far, -1)
    plan(15.0, q_far, 1)
    plan(18.6, q_far, 2)
    plan(6.6, sib_arrive, 0)
    plan(6.6, col_squares, 0)
    plan(9.1, row_squares, 0)
    plan(12.6, sib_arrive, 1)
    plan(12.6, col_squares, 1)
    plan(12.6, col_squares, -1)
    plan(15.6, row_squares, 1)
    plan(15.6, row_squares, -1)
    plan(17.1, sib_arrive, 2)
    plan(17.1, col_squares, 2)
    plan(17.1, col_squares, -2)
    plan(18.6, row_squares, 2)
    plan(18.6, tile, 0)
    plan(19.9, tile, 1, -1)
    plan(22.605, tile, 2, -2)
    plan(22.61, sib_arrive, 3)
    plan(22.62, col_squares, 3)
    plan(22.63, col_squares, -3)
    plan(22.64, tile, 3, -3)
    for _, _, what, args in sorted(events, key=lambda e: e[:2]):
        what(*args)
    sib_arrive(4)
    col_squares(4)
    tile(4)

    z_order = [(d, k) for d in (4, 3, -3, 2, -2, 1, -1, 0) for k in (1, 0) if d or k]
    pq_order = sorted(
        ((i, j) for i in range(4) for j in range(4) if i or j),
        key=lambda d: -min(d[0], 4 - d[0]) - min(d[1], 4 - d[1]),
    )
    z_peers = [at_z(zmod(d), c + k - 2 * c * k) for d, k in z_order]
    pq_peers = [at_pq(pmod(i), qmod(j)) for i, j in pq_order]

    def exchange(buf, me, peers):
        k = len(used)
        for dev in peers:
            pltpu.make_async_remote_copy(
                src_ref=buf.at[me], dst_ref=buf.at[me], send_sem=xs.at[k], recv_sem=xr.at[k],
                device_id=dev, device_id_type=MESH,
            ).start()
        used.append((k, buf))

        def wait():
            some = buf.at[pl.ds(0, 15)]
            pltpu.make_async_copy(some, some, xr.at[k]).wait()

        return wait

    def joined(buf):
        peak = buf[0]
        for k in range(1, 16):
            peak = jnp.maximum(peak, buf[k])
        total = jnp.exp(buf[0] - peak)
        for k in range(1, 16):
            total = total + jnp.exp(buf[k] - peak)
        return peak + jnp.log(total)

    def in_line(v):
        return jnp.concatenate([v[j : j + 1, :] for j in range(NZ)], axis=1)

    columns_known = exchange(cstat, zc, z_peers)
    cown[...] = cstat[zc]

    def row_stats(k, carry):
        part = pl.ds(pl.multiple_of(k * 128, 128), 128)
        block = logits[part, :]
        peak = jnp.max(block, axis=1, keepdims=True)
        total = peak + jnp.log(jnp.sum(jnp.exp(block - peak), axis=1, keepdims=True))
        rvec[part, :] = 0.5 * total
        rstat[own, pl.ds(k, 1), :] = to_lanes(total)
        return carry

    lax.fori_loop(0, 4, row_stats, 0)
    rows_known = exchange(rstat, own, pq_peers)

    def start_halves(k, carry):
        part = pl.ds(pl.multiple_of(k * 128, 128), 128)
        logits[part, :] = jnp.exp(logits[part, :] - rvec[part, :] - 0.5 * in_line(cown[...]))
        return carry

    lax.fori_loop(0, 4, start_halves, 0)
    columns_known()
    cown[...] = jnp.exp(0.5 * (cown[...] - joined(cstat)))
    lane_id = lax.broadcasted_iota(jnp.int32, (1, CHUNK), 1)
    is_real = lax.rem(lane_id // PER, 2) == 1

    def masses(k, carry):
        part = pl.ds(pl.multiple_of(k * 128, 128), 128)
        total = logits[part, 0:CHUNK] * cown[0:1, :]
        for j in range(1, NZ):
            total = total + logits[part, j * CHUNK : (j + 1) * CHUNK] * cown[j : j + 1, :]
        real = jnp.sum(jnp.where(is_real, total, 0.0), axis=1, keepdims=True)
        gen = jnp.sum(jnp.where(is_real, 0.0, total), axis=1, keepdims=True)
        mstat[own, pl.ds(k, 1), :] = to_lanes(gen)
        mstat[own, pl.ds(4 + k, 1), :] = to_lanes(real)
        return carry

    lax.fori_loop(0, 4, masses, 0)
    masses_known = exchange(mstat, own, pq_peers)
    rows_known()
    joint = joined(rstat)
    shares = [jnp.exp(0.5 * (rstat[k] - joint)) for k in range(16)]
    my_share = jnp.exp(0.5 * (rstat[own] - joint))
    masses_known()
    gen = shares[0] * mstat[0, 0:4]
    real = shares[0] * mstat[0, 4:8]
    for k in range(1, 16):
        gen = gen + shares[k] * mstat[k, 0:4]
        real = real + shares[k] * mstat[k, 4:8]
    mstat[16, 0:4] = my_share * gen
    mstat[16, 4:8] = -my_share * real

    def weigh(qq, at):
        part = pl.ds(pl.multiple_of(qq * 128, 128), 128)
        on_real = to_rows(mstat[16, pl.ds(qq, 1), :])
        on_gen = to_rows(mstat[16, pl.ds(qq + 4, 1), :])
        scale = jnp.where(is_real, on_real, on_gen)
        for j in range(NZ):
            half = logits[part, j * CHUNK : (j + 1) * CHUNK] * cown[j : j + 1, :]
            weights[at, :, j * CHUNK : (j + 1) * CHUNK] = (half * scale).astype(BF16)

    def lanes(s):
        return pl.ds(pl.multiple_of(s * PIECE, PIECE), PIECE)

    def drift(w, s):
        samples = cols[:, :, :, :, lanes(s)].reshape(COLS, PIECE)
        return jnp.dot(w, samples, preferred_element_type=F32)

    def each(body):
        def one(s, carry):
            body(s)
            return carry
        lax.fori_loop(0, SLICES, one, 0)

    far_sem = len(index)
    near_sem, last_sem = far_sem + SLICES, far_sem + 2 * SLICES
    assert last_sem + SLICES == SEMS

    before, after, across = qmod(-1), qmod(1), qmod(2)
    ahead, behind = at_pq(p, after), at_pq(p, before)
    lo, hi = pl.ds(0, 2), pl.ds(2, 2)
    weigh(across, 0)

    def far_part(s):
        psend[s, 0] = drift(weights[0], s).reshape(4, PER, PIECE).astype(BF16)
        post(far_sem + s, "f", psend.at[s, 0, lo], far.at[s, 0], ahead)
        post(far_sem + s, "f", psend.at[s, 0, hi], far.at[s, 1], behind)

    each(far_part)
    weigh(after, 1)
    weigh(before, 2)

    def near_part(s):
        part = drift(weights[1:3].reshape(256, COLS), s).reshape(8, PER, PIECE)
        psend[s, 1, 2:4] = part[2:4].astype(BF16)
        post(near_sem + s, "f", psend.at[s, 1, hi], near.at[s, 0, hi], ahead)
        psend[s, 2, 0:2] = part[4:6].astype(BF16)
        post(near_sem + s, "f", psend.at[s, 2, lo], near.at[s, 1, lo], behind)
        kept[s, 0:2] = part[0:2]
        kept[s, 2:4] = part[6:8]

    each(near_part)
    weigh(q, 0)

    def own_part(s):
        acc[s] = drift(weights[0], s).reshape(4, PER, PIECE)

    each(own_part)

    def relay(s):
        pltpu.make_async_copy(far.at[s], far.at[s], rsem.at[far_sem + s]).wait()
        psend[s, 1, 0:2] = (kept[s, 0:2] + far[s, 0].astype(F32)).astype(BF16)
        post(near_sem + s, "f", psend.at[s, 1, lo], near.at[s, 0, lo], ahead)
        psend[s, 2, 2:4] = (kept[s, 2:4] + far[s, 1].astype(F32)).astype(BF16)
        post(near_sem + s, "f", psend.at[s, 2, hi], near.at[s, 1, hi], behind)

    each(relay)

    def last_part(s):
        pltpu.make_async_copy(near.at[s], near.at[s], rsem.at[near_sem + s]).wait()
        for d in (2, 1, 3):
            k = pmod(d)
            total = acc[s, k] + near[s, 0, k].astype(F32) + near[s, 1, k].astype(F32)
            qsend[s, d - 1] = total.astype(BF16)
            post(last_sem + s, "r", qsend.at[s, d - 1], qrecv.at[s, d - 1], at_pq(k, q))

    each(last_part)

    def finish(s, square):
        total = acc[s, p] + near[s, 0, p].astype(F32) + near[s, 1, p].astype(F32)
        pltpu.make_async_copy(qrecv.at[s], qrecv.at[s], rsem.at[last_sem + s]).wait()
        for d in (1, 3, 2):
            total = total + qrecv[s, d - 1].astype(F32)
        out_ref[:, lanes(s)] = total
        for k in range(PIECE // 128):
            lane = total[:, k * 128 : (k + 1) * 128]
            square = square + lane * lane
        return square

    square = lax.fori_loop(0, SLICES, finish, jnp.zeros((PER, 128), F32))
    n1[zc] = jnp.broadcast_to(jnp.sum(square, keepdims=True), (1, 128))
    first_known = exchange(n1, zc, z_peers)
    first_known()
    total = n1[0]
    for k in range(1, 16):
        total = total + n1[k]
    n2[own] = total
    second_known = exchange(n2, own, pq_peers)
    second_known()
    total = n2[0]
    for k in range(1, 16):
        total = total + n2[k]
    count = NX * NY * NZ * NC * PER * WIDTH
    out_ref[...] = out_ref[...] * lax.rsqrt(total / count + EPS)[0:1, 0:1]
    drain()


def on_device(gen, real):
    dma = pltpu.SemaphoreType.DMA
    return pl.pallas_call(
        kernel,
        out_shape=jax.ShapeDtypeStruct((PER, WIDTH), F32),
        in_specs=[pl.BlockSpec(memory_space=pl.ANY)] * 2,
        out_specs=pl.BlockSpec(memory_space=pltpu.VMEM),
        scratch_shapes=[
            pltpu.VMEM((16, PER, WIDTH), BF16),
            pltpu.VMEM((NZ, NC, 2, PER, WIDTH), BF16),
            pltpu.VMEM((ROWS, COLS), F32),
            pltpu.VMEM((ROWS, CHUNK), F32),
            pltpu.VMEM((ROWS, 1), F32),
            pltpu.VMEM((NZ, CHUNK), F32),
            pltpu.VMEM((NZ, CHUNK), F32),
            pltpu.VMEM((16, NZ, CHUNK), F32),
            pltpu.VMEM((16, 4, 128), F32),
            pltpu.VMEM((17, 8, 128), F32),
            pltpu.VMEM((16, 1, 128), F32),
            pltpu.VMEM((16, 1, 128), F32),
            pltpu.VMEM((3, 128, COLS), BF16),
            pltpu.VMEM((SLICES, 3, 4, PER, PIECE), BF16),
            pltpu.VMEM((SLICES, 4, PER, PIECE), F32),
            pltpu.VMEM((SLICES, 4, PER, PIECE), F32),
            pltpu.VMEM((SLICES, 2, 2, PER, PIECE), BF16),
            pltpu.VMEM((SLICES, 2, 4, PER, PIECE), BF16),
            pltpu.VMEM((SLICES, 3, PER, PIECE), BF16),
            pltpu.VMEM((SLICES, 3, PER, PIECE), BF16),
            dma, dma((5,)), dma((SEMS,)), dma((5,)), dma((5,)),
        ],
        compiler_params=pltpu.CompilerParams(
            collective_id=0, has_side_effects=True, vmem_limit_bytes=60 * 1024 * 1024
        ),
    )(gen, real)


def solution(mesh):
    torus = Mesh(mesh.devices.reshape(NZ, NY, NC, NX), AXES)
    return jax.shard_map(
        on_device,
        mesh=torus,
        in_specs=(P(AXES, None), P(AXES, None)),
        out_specs=P(AXES, None),
        check_vma=False,
    )
```

```python
import jax
import jax.numpy as jnp
from jax import lax
from jax.experimental import pallas as pl
from jax.experimental.pallas import tpu as pltpu
from jax.sharding import Mesh
from jax.sharding import PartitionSpec as P

AXES = ("z", "y", "c", "x")
NZ, NY, NC, NX = 8, 4, 2, 4
PER = 32
HALF = PER // 2
WIDTH = 2048
ROWS = NX * NY * PER
CHUNK = 2 * NC * PER
COLS = NZ * CHUNK
SLICES = 2
PIECE = WIDTH // SLICES
INV_SCALE = 1.0 / 0.3
MASKED = -1e30
EPS = 1e-6
F32 = jnp.float32
BF16 = jnp.bfloat16
MESH = pl.DeviceIdType.MESH
SEMS = 35


def eye():
    return lax.broadcasted_iota(jnp.int32, (128, 128), 0) == lax.broadcasted_iota(
        jnp.int32, (128, 128), 1
    )


def to_lanes(v):
    return jnp.sum(jnp.where(eye(), jnp.broadcast_to(v, (128, 128)), 0.0), axis=0, keepdims=True)


def to_rows(v):
    return jnp.sum(jnp.where(eye(), jnp.broadcast_to(v, (128, 128)), 0.0), axis=1, keepdims=True)


def kernel(
    gen_ref, real_ref, out_ref,
    rows, cols, logits, rsq, rvec, csq, cown,
    cstat, rstat, mstat, n1, n2,
    weights, psend, acc, kept, far, near, qsend, qrecv,
    in_sem, ssem, rsem, xs, xr,
):
    z, y, c, x = (lax.axis_index(a) for a in AXES)
    p = x * (1 - c) + y * c
    q = y * (1 - c) + x * c

    def at_z(zz, cc=c):
        return {"z": zz, "y": y, "c": cc, "x": x}

    def at_pq(pp, qq):
        return {"z": z, "y": qq * (1 - c) + pp * c, "c": c, "x": pp * (1 - c) + qq * c}

    def zmod(d):
        return lax.rem(z + (d + NZ), NZ)

    def pmod(d):
        return lax.rem(p + (d + 4), 4)

    def qmod(d):
        return lax.rem(q + (d + 4), 4)

    sibling = at_z(z, 1 - c)
    used, index = [], {}
    kinds = ("z", "s", "p", "f", "r")

    def drain():
        sent = (rows.at[pl.ds(0, 14)], rows, rows.at[pl.ds(0, 15)], psend, qsend)
        for k, ref in enumerate(sent):
            pltpu.make_async_copy(ref, ref, ssem.at[k]).wait()
        for k, buf in used:
            some = buf.at[pl.ds(0, 15)]
            pltpu.make_async_copy(some, some, xs.at[k]).wait()

    def post(k, kind, src, dst, dev):
        pltpu.make_async_remote_copy(
            src_ref=src, dst_ref=dst, send_sem=ssem.at[kinds.index(kind)], recv_sem=rsem.at[k],
            device_id=dev, device_id_type=MESH,
        ).start()

    def send(key, src, dst, dev):
        k = index.setdefault(key, len(index))
        post(k, {"q": "p"}.get(key[0][0], key[0][0]), src, dst, dev)

    def arrived(key, ref):
        pltpu.make_async_copy(ref, ref, rsem.at[index[key]]).wait()

    own = q * 4 + p
    loads = (
        pltpu.make_async_copy(gen_ref, rows.at[own], in_sem),
        pltpu.make_async_copy(gen_ref, cols.at[z, c, 0], in_sem),
        pltpu.make_async_copy(real_ref, cols.at[z, c, 1], in_sem),
    )
    for copy in loads:
        copy.start()
    barrier = pltpu.get_barrier_semaphore()
    around = (
        sibling, at_z(zmod(1)), at_z(zmod(-1)),
        at_pq(pmod(1), q), at_pq(pmod(-1), q), at_pq(p, qmod(1)), at_pq(p, qmod(-1)),
    )
    for dev in around:
        pl.semaphore_signal(barrier, inc=1, device_id=dev, device_id_type=MESH)
    pl.semaphore_wait(barrier, len(around))
    pltpu.make_async_copy(rows.at[pl.ds(0, 3)], rows.at[pl.ds(0, 3)], in_sem).wait()

    top, low = pl.ds(0, HALF), pl.ds(HALF, HALF)

    def z_piece(d, h, j):
        kind = j // 2 if d == 0 else 1 - j // 2
        return cols.at[zmod((2 * d - 1) * h), c, kind, low if j % 2 else top], kind

    def z_send(d, h, j):
        src, _ = z_piece(d, h - 1, j)
        send(("z", h, j), src, src, at_z(zmod(1 - 2 * d)))

    def z_arrive(h, j):
        arrived(("z", h, j), cols.at[0, 0, 0])
        for d in (0, 1):
            if h < 3 or (h == 3 and j < 2):
                z_send(d, h + 1, j)
        for d in (0, 1):
            src, kind = z_piece(d, h, j)
            if h == 4:
                send(("s", h), src, src, sibling)
            elif h < 4 and j % 2:
                whole = cols.at[zmod((2 * d - 1) * h), c, kind]
                send(("s", h), whole, whole, sibling)

    def sib_arrive(h):
        arrived(("s", h), {0: cols.at[0, 0], 4: cols.at[0, 0]}.get(h, cols.at[0]))

    def at_row(dq, dp):
        return qmod(dq) * 4 + pmod(dp)

    def q_sends(dp):
        block = rows.at[at_row(0, dp)]
        send(("q", dp), block, block, at_pq(p, qmod(1)))
        send(("q", dp), block, block, at_pq(p, qmod(-1)))

    def p_arrive():
        arrived(("p",), rows.at[pl.ds(0, 2)])
        for d in (1, -1):
            half = rows.at[at_row(0, -d), top if d > 0 else low]
            send(("pf",), half, half, at_pq(pmod(d), q))
        q_sends(-1)
        q_sends(1)

    def p_far():
        arrived(("pf",), rows.at[0])
        q_sends(2)

    def q_arrive(dp):
        arrived(("q", dp), rows.at[pl.ds(0, 2)])
        for d in (1, -1):
            half = rows.at[at_row(-d, dp), top if d > 0 else low]
            send(("qf", dp), half, half, at_pq(p, qmod(d)))

    def q_far(dp):
        arrived(("qf", dp), rows.at[0])

    def squares_of(value):
        value = value.astype(F32)
        return jnp.sum(value * value, axis=1, keepdims=True)

    def row_squares(dq):
        def one(k, carry):
            g = qmod(dq) * 4 + k
            rsq[pl.ds(g * PER, PER), :] = jnp.broadcast_to(squares_of(rows[g]), (PER, CHUNK))
            return carry
        lax.fori_loop(0, 4, one, 0)

    def col_squares(d):
        csq[pl.ds(zmod(d), 1), :] = to_lanes(squares_of(cols[zmod(d)].reshape(CHUNK, WIDTH)))

    def lanes_of(d):
        return pl.ds(pl.multiple_of(zmod(d) * CHUNK, CHUNK), CHUNK)

    zc = z * NC + c

    def tile(*ds):
        def rhs():
            parts = [cols[zmod(d)].reshape(CHUNK, WIDTH) for d in ds]
            return jnp.concatenate(parts, axis=0) if len(parts) > 1 else parts[0]

        n = 1 if ds == (4,) else 2
        block_rows = ROWS // n

        def some_rows(b, carry):
            part = pl.ds(pl.multiple_of(b * block_rows, block_rows), block_rows)
            lhs = rows[pl.ds(b * (16 // n), 16 // n)].reshape(block_rows, WIDTH)
            inner = lax.dot_general(
                lhs, rhs(), (((1,), (1,)), ((), ())), preferred_element_type=F32
            )
            for k, d in enumerate(ds):
                gap = rsq[part, :] + csq[pl.ds(zmod(d), 1), :]
                gap = jnp.maximum(gap - 2.0 * inner[:, k * CHUNK : (k + 1) * CHUNK], 1.0)
                logits[part, lanes_of(d)] = gap * lax.rsqrt(gap) * -INV_SCALE
            return carry

        lax.fori_loop(0, n, some_rows, 0)
        if ds == (0,):
            mine = pl.ds(pl.multiple_of(own * PER, PER), PER)
            block = logits[mine, lanes_of(0)]
            lane_id = lax.broadcasted_iota(jnp.int32, block.shape, 1)
            row_id = lax.broadcasted_iota(jnp.int32, block.shape, 0)
            logits[mine, lanes_of(0)] = jnp.where(lane_id == row_id + c * 2 * PER, MASKED, block)
        for d in ds:
            block = logits[:, lanes_of(d)]
            peak = jnp.max(block, axis=0, keepdims=True)
            total = jnp.sum(jnp.exp(block - peak), axis=0, keepdims=True)
            cstat[zc, pl.ds(zmod(d), 1), :] = peak + jnp.log(total)

    for j in range(4):
        for d in (0, 1):
            z_send(d, 1, j)
    for d in (1, -1):
        send(("p",), rows.at[own], rows.at[own], at_pq(pmod(d), q))
    q_sends(0)
    for kind in (0, 1):
        send(("s", 0), cols.at[z, c, kind], cols.at[z, c, kind], sibling)

    events = []

    def plan(when, what, *args):
        events.append((when, len(events), what, args))

    for h in range(1, 5):
        for j in range(4 if h < 4 else 2):
            plan(3.0 + 1.4 * ((h - 1) * 4 + j + 1), z_arrive, h, j)
    plan(4.8, p_arrive)
    plan(6.5, q_arrive, 0)
    plan(9.0, p_far)
    plan(10.0, q_arrive, -1)
    plan(11.0, q_arrive, 1)
    plan(11.0, q_far, 0)
    plan(13.9, q_arrive, 2)
    plan(15.0, q_far, -1)
    plan(15.0, q_far, 1)
    plan(18.6, q_far, 2)
    plan(6.6, sib_arrive, 0)
    plan(6.6, col_squares, 0)
    plan(9.1, row_squares, 0)
    plan(12.6, sib_arrive, 1)
    plan(12.6, col_squares, 1)
    plan(12.6, col_squares, -1)
    plan(15.6, row_squares, 1)
    plan(15.6, row_squares, -1)
    plan(17.1, sib_arrive, 2)
    plan(17.1, col_squares, 2)
    plan(17.1, col_squares, -2)
    plan(18.6, row_squares, 2)
    plan(18.6, tile, 0)
    plan(19.9, tile, 1, -1)
    plan(22.605, tile, 2, -2)
    plan(22.61, sib_arrive, 3)
    plan(22.62, col_squares, 3)
    plan(22.63, col_squares, -3)
    plan(22.64, tile, 3, -3)
    for _, _, what, args in sorted(events, key=lambda e: e[:2]):
        what(*args)
    sib_arrive(4)
    col_squares(4)
    tile(4)

    z_order = [(d, k) for d in (4, 3, -3, 2, -2, 1, -1, 0) for k in (0, 1) if d or k]
    pq_order = sorted(
        ((i, j) for i in range(4) for j in range(4) if i or j),
        key=lambda d: -min(d[0], 4 - d[0]) - min(d[1], 4 - d[1]),
    )
    z_peers = [at_z(zmod(d), c + k - 2 * c * k) for d, k in z_order]
    pq_peers = [at_pq(pmod(i), qmod(j)) for i, j in pq_order]

    def exchange(buf, me, peers):
        k = len(used)
        for dev in peers:
            pltpu.make_async_remote_copy(
                src_ref=buf.at[me], dst_ref=buf.at[me], send_sem=xs.at[k], recv_sem=xr.at[k],
                device_id=dev, device_id_type=MESH,
            ).start()
        used.append((k, buf))

        def wait():
            some = buf.at[pl.ds(0, 15)]
            pltpu.make_async_copy(some, some, xr.at[k]).wait()

        return wait

    def joined(buf):
        peak = buf[0]
        for k in range(1, 16):
            peak = jnp.maximum(peak, buf[k])
        total = jnp.exp(buf[0] - peak)
        for k in range(1, 16):
            total = total + jnp.exp(buf[k] - peak)
        return peak + jnp.log(total)

    def in_line(v):
        return jnp.concatenate([v[j : j + 1, :] for j in range(NZ)], axis=1)

    columns_known = exchange(cstat, zc, z_peers)
    cown[...] = cstat[zc]

    def row_stats(k, carry):
        part = pl.ds(pl.multiple_of(k * 128, 128), 128)
        block = logits[part, :]
        peak = jnp.max(block, axis=1, keepdims=True)
        total = peak + jnp.log(jnp.sum(jnp.exp(block - peak), axis=1, keepdims=True))
        rvec[part, :] = 0.5 * total
        rstat[own, pl.ds(k, 1), :] = to_lanes(total)
        return carry

    lax.fori_loop(0, 4, row_stats, 0)
    rows_known = exchange(rstat, own, pq_peers)

    def start_halves(k, carry):
        part = pl.ds(pl.multiple_of(k * 128, 128), 128)
        logits[part, :] = jnp.exp(logits[part, :] - rvec[part, :] - 0.5 * in_line(cown[...]))
        return carry

    lax.fori_loop(0, 4, start_halves, 0)
    columns_known()
    cown[...] = jnp.exp(0.5 * (cown[...] - joined(cstat)))
    lane_id = lax.broadcasted_iota(jnp.int32, (1, CHUNK), 1)
    is_real = lax.rem(lane_id // PER, 2) == 1

    def masses(k, carry):
        part = pl.ds(pl.multiple_of(k * 128, 128), 128)
        total = logits[part, 0:CHUNK] * cown[0:1, :]
        for j in range(1, NZ):
            total = total + logits[part, j * CHUNK : (j + 1) * CHUNK] * cown[j : j + 1, :]
        real = jnp.sum(jnp.where(is_real, total, 0.0), axis=1, keepdims=True)
        gen = jnp.sum(jnp.where(is_real, 0.0, total), axis=1, keepdims=True)
        mstat[own, pl.ds(k, 1), :] = to_lanes(gen)
        mstat[own, pl.ds(4 + k, 1), :] = to_lanes(real)
        return carry

    lax.fori_loop(0, 4, masses, 0)
    masses_known = exchange(mstat, own, pq_peers)
    rows_known()
    joint = joined(rstat)
    shares = [jnp.exp(0.5 * (rstat[k] - joint)) for k in range(16)]
    my_share = jnp.exp(0.5 * (rstat[own] - joint))
    masses_known()
    gen = shares[0] * mstat[0, 0:4]
    real = shares[0] * mstat[0, 4:8]
    for k in range(1, 16):
        gen = gen + shares[k] * mstat[k, 0:4]
        real = real + shares[k] * mstat[k, 4:8]
    mstat[16, 0:4] = my_share * gen
    mstat[16, 4:8] = -my_share * real

    def weigh(qq, at):
        part = pl.ds(pl.multiple_of(qq * 128, 128), 128)
        on_real = to_rows(mstat[16, pl.ds(qq, 1), :])
        on_gen = to_rows(mstat[16, pl.ds(qq + 4, 1), :])
        scale = jnp.where(is_real, on_real, on_gen)
        for j in range(NZ):
            half = logits[part, j * CHUNK : (j + 1) * CHUNK] * cown[j : j + 1, :]
            weights[at, :, j * CHUNK : (j + 1) * CHUNK] = (half * scale).astype(BF16)

    def lanes(s):
        return pl.ds(pl.multiple_of(s * PIECE, PIECE), PIECE)

    def drift(w, s):
        samples = cols[:, :, :, :, lanes(s)].reshape(COLS, PIECE)
        return jnp.dot(w, samples, preferred_element_type=F32)

    def each(body):
        def one(s, carry):
            body(s)
            return carry
        lax.fori_loop(0, SLICES, one, 0)

    far_sem = len(index)
    near_sem, last_sem = far_sem + SLICES, far_sem + 2 * SLICES
    assert last_sem + SLICES == SEMS

    before, after, across = qmod(-1), qmod(1), qmod(2)
    ahead, behind = at_pq(p, after), at_pq(p, before)
    lo, hi = pl.ds(0, 2), pl.ds(2, 2)
    weigh(across, 0)

    def far_part(s):
        psend[s, 0] = drift(weights[0], s).reshape(4, PER, PIECE).astype(BF16)
        post(far_sem + s, "f", psend.at[s, 0, lo], far.at[s, 0], ahead)
        post(far_sem + s, "f", psend.at[s, 0, hi], far.at[s, 1], behind)

    each(far_part)
    weigh(after, 1)
    weigh(before, 2)

    def near_part(s):
        part = drift(weights[1:3].reshape(256, COLS), s).reshape(8, PER, PIECE)
        psend[s, 1, 2:4] = part[2:4].astype(BF16)
        post(near_sem + s, "f", psend.at[s, 1, hi], near.at[s, 0, hi], ahead)
        psend[s, 2, 0:2] = part[4:6].astype(BF16)
        post(near_sem + s, "f", psend.at[s, 2, lo], near.at[s, 1, lo], behind)
        kept[s, 0:2] = part[0:2]
        kept[s, 2:4] = part[6:8]

    each(near_part)
    weigh(q, 0)

    def own_part(s):
        acc[s] = drift(weights[0], s).reshape(4, PER, PIECE)


    def relay(s):
        pltpu.make_async_copy(far.at[s], far.at[s], rsem.at[far_sem + s]).wait()
        psend[s, 1, 0:2] = (kept[s, 0:2] + far[s, 0].astype(F32)).astype(BF16)
        post(near_sem + s, "f", psend.at[s, 1, lo], near.at[s, 0, lo], ahead)
        psend[s, 2, 2:4] = (kept[s, 2:4] + far[s, 1].astype(F32)).astype(BF16)
        post(near_sem + s, "f", psend.at[s, 2, hi], near.at[s, 1, hi], behind)

    def relay_then_own(s):
        relay(s)
        own_part(s)

    each(relay_then_own)

    def last_part(s):
        pltpu.make_async_copy(near.at[s], near.at[s], rsem.at[near_sem + s]).wait()
        for d in (2, 1, 3):
            k = pmod(d)
            total = acc[s, k] + near[s, 0, k].astype(F32) + near[s, 1, k].astype(F32)
            qsend[s, d - 1] = total.astype(BF16)
            post(last_sem + s, "r", qsend.at[s, d - 1], qrecv.at[s, d - 1], at_pq(k, q))

    each(last_part)

    def finish(s, square):
        total = acc[s, p] + near[s, 0, p].astype(F32) + near[s, 1, p].astype(F32)
        pltpu.make_async_copy(qrecv.at[s], qrecv.at[s], rsem.at[last_sem + s]).wait()
        for d in (1, 3, 2):
            total = total + qrecv[s, d - 1].astype(F32)
        out_ref[:, lanes(s)] = total
        for k in range(PIECE // 128):
            lane = total[:, k * 128 : (k + 1) * 128]
            square = square + lane * lane
        return square

    square = lax.fori_loop(0, SLICES, finish, jnp.zeros((PER, 128), F32))
    n1[zc] = jnp.broadcast_to(jnp.sum(square, keepdims=True), (1, 128))
    first_known = exchange(n1, zc, z_peers)
    first_known()
    total = n1[0]
    for k in range(1, 16):
        total = total + n1[k]
    n2[own] = total
    second_known = exchange(n2, own, pq_peers)
    second_known()
    total = n2[0]
    for k in range(1, 16):
        total = total + n2[k]
    count = NX * NY * NZ * NC * PER * WIDTH
    out_ref[...] = out_ref[...] * lax.rsqrt(total / count + EPS)[0:1, 0:1]
    drain()


def on_device(gen, real):
    dma = pltpu.SemaphoreType.DMA
    return pl.pallas_call(
        kernel,
        out_shape=jax.ShapeDtypeStruct((PER, WIDTH), F32),
        in_specs=[pl.BlockSpec(memory_space=pl.ANY)] * 2,
        out_specs=pl.BlockSpec(memory_space=pltpu.VMEM),
        scratch_shapes=[
            pltpu.VMEM((16, PER, WIDTH), BF16),
            pltpu.VMEM((NZ, NC, 2, PER, WIDTH), BF16),
            pltpu.VMEM((ROWS, COLS), F32),
            pltpu.VMEM((ROWS, CHUNK), F32),
            pltpu.VMEM((ROWS, 1), F32),
            pltpu.VMEM((NZ, CHUNK), F32),
            pltpu.VMEM((NZ, CHUNK), F32),
            pltpu.VMEM((16, NZ, CHUNK), F32),
            pltpu.VMEM((16, 4, 128), F32),
            pltpu.VMEM((17, 8, 128), F32),
            pltpu.VMEM((16, 1, 128), F32),
            pltpu.VMEM((16, 1, 128), F32),
            pltpu.VMEM((3, 128, COLS), BF16),
            pltpu.VMEM((SLICES, 3, 4, PER, PIECE), BF16),
            pltpu.VMEM((SLICES, 4, PER, PIECE), F32),
            pltpu.VMEM((SLICES, 4, PER, PIECE), F32),
            pltpu.VMEM((SLICES, 2, 2, PER, PIECE), BF16),
            pltpu.VMEM((SLICES, 2, 4, PER, PIECE), BF16),
            pltpu.VMEM((SLICES, 3, PER, PIECE), BF16),
            pltpu.VMEM((SLICES, 3, PER, PIECE), BF16),
            dma, dma((5,)), dma((SEMS,)), dma((5,)), dma((5,)),
        ],
        compiler_params=pltpu.CompilerParams(
            collective_id=0, has_side_effects=True, vmem_limit_bytes=60 * 1024 * 1024
        ),
    )(gen, real)


def solution(mesh):
    torus = Mesh(mesh.devices.reshape(NZ, NY, NC, NX), AXES)
    return jax.shard_map(
        on_device,
        mesh=torus,
        in_specs=(P(AXES, None), P(AXES, None)),
        out_specs=P(AXES, None),
        check_vma=False,
    )
```

```python
import jax
import jax.numpy as jnp
from jax import lax
from jax.experimental import pallas as pl
from jax.experimental.pallas import tpu as pltpu
from jax.sharding import Mesh
from jax.sharding import PartitionSpec as P

AXES = ("z", "y", "c", "x")
NZ, NY, NC, NX = 8, 4, 2, 4
PER = 32
HALF = PER // 2
WIDTH = 2048
ROWS = NX * NY * PER
CHUNK = 2 * NC * PER
COLS = NZ * CHUNK
SLICES = 2
PIECE = WIDTH // SLICES
INV_SCALE = 1.0 / 0.3
MASKED = -1e30
EPS = 1e-6
F32 = jnp.float32
BF16 = jnp.bfloat16
MESH = pl.DeviceIdType.MESH
SEMS = 35


def eye():
    return lax.broadcasted_iota(jnp.int32, (128, 128), 0) == lax.broadcasted_iota(
        jnp.int32, (128, 128), 1
    )


def to_lanes(v):
    return jnp.sum(jnp.where(eye(), jnp.broadcast_to(v, (128, 128)), 0.0), axis=0, keepdims=True)


def to_rows(v):
    return jnp.sum(jnp.where(eye(), jnp.broadcast_to(v, (128, 128)), 0.0), axis=1, keepdims=True)


def kernel(
    gen_ref, real_ref, out_ref,
    rows, cols, logits, rsq, rvec, csq, cown,
    cstat, rstat, mstat, n1, n2,
    weights, psend, acc, kept, far, near, qsend, qrecv,
    in_sem, ssem, rsem, xs, xr,
):
    z, y, c, x = (lax.axis_index(a) for a in AXES)
    p = x * (1 - c) + y * c
    q = y * (1 - c) + x * c

    def at_z(zz, cc=c):
        return {"z": zz, "y": y, "c": cc, "x": x}

    def at_pq(pp, qq):
        return {"z": z, "y": qq * (1 - c) + pp * c, "c": c, "x": pp * (1 - c) + qq * c}

    def zmod(d):
        return lax.rem(z + (d + NZ), NZ)

    def pmod(d):
        return lax.rem(p + (d + 4), 4)

    def qmod(d):
        return lax.rem(q + (d + 4), 4)

    sibling = at_z(z, 1 - c)
    used, index = [], {}
    kinds = ("z", "s", "p", "f", "r")

    def drain():
        sent = (rows.at[pl.ds(0, 14)], rows, rows.at[pl.ds(0, 15)], psend, qsend)
        for k, ref in enumerate(sent):
            pltpu.make_async_copy(ref, ref, ssem.at[k]).wait()
        for k, buf in used:
            some = buf.at[pl.ds(0, 15)]
            pltpu.make_async_copy(some, some, xs.at[k]).wait()

    def post(k, kind, src, dst, dev):
        pltpu.make_async_remote_copy(
            src_ref=src, dst_ref=dst, send_sem=ssem.at[kinds.index(kind)], recv_sem=rsem.at[k],
            device_id=dev, device_id_type=MESH,
        ).start()

    def send(key, src, dst, dev):
        k = index.setdefault(key, len(index))
        post(k, {"q": "p"}.get(key[0][0], key[0][0]), src, dst, dev)

    def arrived(key, ref):
        pltpu.make_async_copy(ref, ref, rsem.at[index[key]]).wait()

    own = q * 4 + p
    loads = (
        pltpu.make_async_copy(gen_ref, rows.at[own], in_sem),
        pltpu.make_async_copy(gen_ref, cols.at[z, c, 0], in_sem),
        pltpu.make_async_copy(real_ref, cols.at[z, c, 1], in_sem),
    )
    for copy in loads:
        copy.start()
    barrier = pltpu.get_barrier_semaphore()
    around = (
        sibling, at_z(zmod(1)), at_z(zmod(-1)),
        at_pq(pmod(1), q), at_pq(pmod(-1), q), at_pq(p, qmod(1)), at_pq(p, qmod(-1)),
    )
    for dev in around:
        pl.semaphore_signal(barrier, inc=1, device_id=dev, device_id_type=MESH)
    pl.semaphore_wait(barrier, len(around))
    pltpu.make_async_copy(rows.at[pl.ds(0, 3)], rows.at[pl.ds(0, 3)], in_sem).wait()

    top, low = pl.ds(0, HALF), pl.ds(HALF, HALF)

    def z_piece(d, h, j):
        kind = j // 2 if d == 0 else 1 - j // 2
        return cols.at[zmod((2 * d - 1) * h), c, kind, low if j % 2 else top], kind

    def z_send(d, h, j):
        src, _ = z_piece(d, h - 1, j)
        send(("z", h, j), src, src, at_z(zmod(1 - 2 * d)))

    def z_arrive(h, j):
        arrived(("z", h, j), cols.at[0, 0, 0])
        for d in (0, 1):
            if h < 3 or (h == 3 and j < 2):
                z_send(d, h + 1, j)
        for d in (0, 1):
            src, kind = z_piece(d, h, j)
            if h == 4:
                send(("s", h), src, src, sibling)
            elif h < 4 and j % 2:
                whole = cols.at[zmod((2 * d - 1) * h), c, kind]
                send(("s", h), whole, whole, sibling)

    def sib_arrive(h):
        arrived(("s", h), {0: cols.at[0, 0], 4: cols.at[0, 0]}.get(h, cols.at[0]))

    def at_row(dq, dp):
        return qmod(dq) * 4 + pmod(dp)

    def q_sends(dp):
        block = rows.at[at_row(0, dp)]
        send(("q", dp), block, block, at_pq(p, qmod(1)))
        send(("q", dp), block, block, at_pq(p, qmod(-1)))

    def p_arrive():
        arrived(("p",), rows.at[pl.ds(0, 2)])
        for d in (1, -1):
            half = rows.at[at_row(0, -d), top if d > 0 else low]
            send(("pf",), half, half, at_pq(pmod(d), q))
        q_sends(-1)
        q_sends(1)

    def p_far():
        arrived(("pf",), rows.at[0])
        q_sends(2)

    def q_arrive(dp):
        arrived(("q", dp), rows.at[pl.ds(0, 2)])
        for d in (1, -1):
            half = rows.at[at_row(-d, dp), top if d > 0 else low]
            send(("qf", dp), half, half, at_pq(p, qmod(d)))

    def q_far(dp):
        arrived(("qf", dp), rows.at[0])

    def squares_of(value):
        value = value.astype(F32)
        return jnp.sum(value * value, axis=1, keepdims=True)

    def row_squares(dq):
        def one(k, carry):
            g = qmod(dq) * 4 + k
            rsq[pl.ds(g * PER, PER), :] = jnp.broadcast_to(squares_of(rows[g]), (PER, CHUNK))
            return carry
        lax.fori_loop(0, 4, one, 0)

    def col_squares(d):
        csq[pl.ds(zmod(d), 1), :] = to_lanes(squares_of(cols[zmod(d)].reshape(CHUNK, WIDTH)))

    def lanes_of(d):
        return pl.ds(pl.multiple_of(zmod(d) * CHUNK, CHUNK), CHUNK)

    zc = z * NC + c

    def tile(*ds):
        def rhs():
            parts = [cols[zmod(d)].reshape(CHUNK, WIDTH) for d in ds]
            return jnp.concatenate(parts, axis=0) if len(parts) > 1 else parts[0]

        n = 1 if ds == (4,) else 2
        block_rows = ROWS // n

        def some_rows(b, carry):
            part = pl.ds(pl.multiple_of(b * block_rows, block_rows), block_rows)
            lhs = rows[pl.ds(b * (16 // n), 16 // n)].reshape(block_rows, WIDTH)
            inner = lax.dot_general(
                lhs, rhs(), (((1,), (1,)), ((), ())), preferred_element_type=F32
            )
            for k, d in enumerate(ds):
                gap = rsq[part, :] + csq[pl.ds(zmod(d), 1), :]
                gap = jnp.maximum(gap - 2.0 * inner[:, k * CHUNK : (k + 1) * CHUNK], 1.0)
                logits[part, lanes_of(d)] = gap * lax.rsqrt(gap) * -INV_SCALE
            return carry

        lax.fori_loop(0, n, some_rows, 0)
        if ds == (0,):
            mine = pl.ds(pl.multiple_of(own * PER, PER), PER)
            block = logits[mine, lanes_of(0)]
            lane_id = lax.broadcasted_iota(jnp.int32, block.shape, 1)
            row_id = lax.broadcasted_iota(jnp.int32, block.shape, 0)
            logits[mine, lanes_of(0)] = jnp.where(lane_id == row_id + c * 2 * PER, MASKED, block)
        for d in ds:
            block = logits[:, lanes_of(d)]
            peak = jnp.max(block, axis=0, keepdims=True)
            total = jnp.sum(jnp.exp(block - peak), axis=0, keepdims=True)
            cstat[zc, pl.ds(zmod(d), 1), :] = peak + jnp.log(total)

    for j in range(4):
        for d in (0, 1):
            z_send(d, 1, j)
    for d in (1, -1):
        send(("p",), rows.at[own], rows.at[own], at_pq(pmod(d), q))
    q_sends(0)
    for kind in (0, 1):
        send(("s", 0), cols.at[z, c, kind], cols.at[z, c, kind], sibling)

    events = []

    def plan(when, what, *args):
        events.append((when, len(events), what, args))

    for h in range(1, 5):
        for j in range(4 if h < 4 else 2):
            plan(3.0 + 1.4 * ((h - 1) * 4 + j + 1), z_arrive, h, j)
    plan(4.8, p_arrive)
    plan(6.5, q_arrive, 0)
    plan(9.0, p_far)
    plan(10.0, q_arrive, -1)
    plan(11.0, q_arrive, 1)
    plan(11.0, q_far, 0)
    plan(13.9, q_arrive, 2)
    plan(15.0, q_far, -1)
    plan(15.0, q_far, 1)
    plan(18.6, q_far, 2)
    plan(6.6, sib_arrive, 0)
    plan(6.6, col_squares, 0)
    plan(9.1, row_squares, 0)
    plan(12.6, sib_arrive, 1)
    plan(12.6, col_squares, 1)
    plan(12.6, col_squares, -1)
    plan(15.6, row_squares, 1)
    plan(15.6, row_squares, -1)
    plan(17.1, sib_arrive, 2)
    plan(17.1, col_squares, 2)
    plan(17.1, col_squares, -2)
    plan(18.6, row_squares, 2)
    plan(18.6, tile, 0)
    plan(19.9, tile, 1, -1)
    plan(22.605, tile, 2, -2)
    plan(22.61, sib_arrive, 3)
    plan(22.62, col_squares, 3)
    plan(22.63, col_squares, -3)
    plan(22.64, tile, 3, -3)
    for _, _, what, args in sorted(events, key=lambda e: e[:2]):
        what(*args)
    sib_arrive(4)
    col_squares(4)
    tile(4)

    z_order = [(d, k) for d in (4, 3, -3, 2, -2, 1, -1, 0) for k in (0, 1) if d or k]
    pq_order = sorted(
        ((i, j) for i in range(4) for j in range(4) if i or j),
        key=lambda d: -min(d[0], 4 - d[0]) - min(d[1], 4 - d[1]),
    )
    z_peers = [at_z(zmod(d), c + k - 2 * c * k) for d, k in z_order]
    pq_peers = [at_pq(pmod(i), qmod(j)) for i, j in pq_order]

    def exchange(buf, me, peers):
        k = len(used)
        for dev in peers:
            pltpu.make_async_remote_copy(
                src_ref=buf.at[me], dst_ref=buf.at[me], send_sem=xs.at[k], recv_sem=xr.at[k],
                device_id=dev, device_id_type=MESH,
            ).start()
        used.append((k, buf))

        def wait():
            some = buf.at[pl.ds(0, 15)]
            pltpu.make_async_copy(some, some, xr.at[k]).wait()

        return wait

    def joined(buf):
        peak = buf[0]
        for k in range(1, 16):
            peak = jnp.maximum(peak, buf[k])
        total = jnp.exp(buf[0] - peak)
        for k in range(1, 16):
            total = total + jnp.exp(buf[k] - peak)
        return peak + jnp.log(total)

    def in_line(v):
        return jnp.concatenate([v[j : j + 1, :] for j in range(NZ)], axis=1)

    columns_known = exchange(cstat, zc, z_peers)
    cown[...] = cstat[zc]

    def row_stats(k, carry):
        part = pl.ds(pl.multiple_of(k * 128, 128), 128)
        block = logits[part, :]
        peak = jnp.max(block, axis=1, keepdims=True)
        total = peak + jnp.log(jnp.sum(jnp.exp(block - peak), axis=1, keepdims=True))
        rvec[part, :] = 0.5 * total
        rstat[own, pl.ds(k, 1), :] = to_lanes(total)
        return carry

    lax.fori_loop(0, 4, row_stats, 0)
    rows_known = exchange(rstat, own, pq_peers)

    def start_halves(k, carry):
        part = pl.ds(pl.multiple_of(k * 128, 128), 128)
        logits[part, :] = jnp.exp(logits[part, :] - rvec[part, :] - 0.5 * in_line(cown[...]))
        return carry

    lax.fori_loop(0, 4, start_halves, 0)
    columns_known()
    cown[...] = jnp.exp(0.5 * (cown[...] - joined(cstat)))
    lane_id = lax.broadcasted_iota(jnp.int32, (1, CHUNK), 1)
    is_real = lax.rem(lane_id // PER, 2) == 1

    def masses(k, carry):
        part = pl.ds(pl.multiple_of(k * 128, 128), 128)
        total = logits[part, 0:CHUNK] * cown[0:1, :]
        for j in range(1, NZ):
            total = total + logits[part, j * CHUNK : (j + 1) * CHUNK] * cown[j : j + 1, :]
        real = jnp.sum(jnp.where(is_real, total, 0.0), axis=1, keepdims=True)
        gen = jnp.sum(jnp.where(is_real, 0.0, total), axis=1, keepdims=True)
        mstat[own, pl.ds(k, 1), :] = to_lanes(gen)
        mstat[own, pl.ds(4 + k, 1), :] = to_lanes(real)
        return carry

    lax.fori_loop(0, 4, masses, 0)
    masses_known = exchange(mstat, own, pq_peers)
    rows_known()
    joint = joined(rstat)
    shares = [jnp.exp(0.5 * (rstat[k] - joint)) for k in range(16)]
    my_share = jnp.exp(0.5 * (rstat[own] - joint))
    masses_known()
    gen = shares[0] * mstat[0, 0:4]
    real = shares[0] * mstat[0, 4:8]
    for k in range(1, 16):
        gen = gen + shares[k] * mstat[k, 0:4]
        real = real + shares[k] * mstat[k, 4:8]
    mstat[16, 0:4] = my_share * gen
    mstat[16, 4:8] = -my_share * real

    def weigh(qq, at):
        part = pl.ds(pl.multiple_of(qq * 128, 128), 128)
        on_real = to_rows(mstat[16, pl.ds(qq, 1), :])
        on_gen = to_rows(mstat[16, pl.ds(qq + 4, 1), :])
        scale = jnp.where(is_real, on_real, on_gen)
        for j in range(NZ):
            half = logits[part, j * CHUNK : (j + 1) * CHUNK] * cown[j : j + 1, :]
            weights[at, :, j * CHUNK : (j + 1) * CHUNK] = (half * scale).astype(BF16)

    def lanes(s):
        return pl.ds(pl.multiple_of(s * PIECE, PIECE), PIECE)

    def drift(w, s):
        samples = cols[:, :, :, :, lanes(s)].reshape(COLS, PIECE)
        return jnp.dot(w, samples, preferred_element_type=F32)

    def each(body):
        def one(s, carry):
            body(s)
            return carry
        lax.fori_loop(0, SLICES, one, 0)

    far_sem = len(index)
    near_sem, last_sem = far_sem + SLICES, far_sem + 2 * SLICES
    assert last_sem + SLICES == SEMS

    before, after, across = qmod(-1), qmod(1), qmod(2)
    ahead, behind = at_pq(p, after), at_pq(p, before)
    lo, hi = pl.ds(0, 2), pl.ds(2, 2)
    weigh(across, 0)

    def far_part(s):
        psend[s, 0] = drift(weights[0], s).reshape(4, PER, PIECE).astype(BF16)
        post(far_sem + s, "f", psend.at[s, 0, lo], far.at[s, 0], ahead)
        post(far_sem + s, "f", psend.at[s, 0, hi], far.at[s, 1], behind)

    each(far_part)
    weigh(after, 1)
    weigh(before, 2)

    def near_part(s):
        part = drift(weights[1:3].reshape(256, COLS), s).reshape(8, PER, PIECE)
        psend[s, 1, 2:4] = part[2:4].astype(BF16)
        post(near_sem + s, "f", psend.at[s, 1, hi], near.at[s, 0, hi], ahead)
        psend[s, 2, 0:2] = part[4:6].astype(BF16)
        post(near_sem + s, "f", psend.at[s, 2, lo], near.at[s, 1, lo], behind)
        kept[s, 0:2] = part[0:2]
        kept[s, 2:4] = part[6:8]

    each(near_part)
    weigh(q, 0)

    def own_part(s):
        acc[s] = drift(weights[0], s).reshape(4, PER, PIECE)


    def relay(s):
        pltpu.make_async_copy(far.at[s], far.at[s], rsem.at[far_sem + s]).wait()
        psend[s, 1, 0:2] = (kept[s, 0:2] + far[s, 0].astype(F32)).astype(BF16)
        post(near_sem + s, "f", psend.at[s, 1, lo], near.at[s, 0, lo], ahead)
        psend[s, 2, 2:4] = (kept[s, 2:4] + far[s, 1].astype(F32)).astype(BF16)
        post(near_sem + s, "f", psend.at[s, 2, hi], near.at[s, 1, hi], behind)

    def relay_then_own(s):
        relay(s)
        own_part(s)

    each(relay_then_own)

    def last_part(s):
        pltpu.make_async_copy(near.at[s], near.at[s], rsem.at[near_sem + s]).wait()
        for d in (1, 3, 2):
            k = pmod(d)
            total = acc[s, k] + near[s, 0, k].astype(F32) + near[s, 1, k].astype(F32)
            qsend[s, d - 1] = total.astype(BF16)
            post(last_sem + s, "r", qsend.at[s, d - 1], qrecv.at[s, d - 1], at_pq(k, q))

    each(last_part)

    def finish(s, square):
        total = acc[s, p] + near[s, 0, p].astype(F32) + near[s, 1, p].astype(F32)
        pltpu.make_async_copy(qrecv.at[s], qrecv.at[s], rsem.at[last_sem + s]).wait()
        for d in (1, 3, 2):
            total = total + qrecv[s, d - 1].astype(F32)
        out_ref[:, lanes(s)] = total
        for k in range(PIECE // 128):
            lane = total[:, k * 128 : (k + 1) * 128]
            square = square + lane * lane
        return square

    square = lax.fori_loop(0, SLICES, finish, jnp.zeros((PER, 128), F32))
    n1[zc] = jnp.broadcast_to(jnp.sum(square, keepdims=True), (1, 128))
    first_known = exchange(n1, zc, z_peers)
    first_known()
    total = n1[0]
    for k in range(1, 16):
        total = total + n1[k]
    n2[own] = total
    second_known = exchange(n2, own, pq_peers)
    second_known()
    total = n2[0]
    for k in range(1, 16):
        total = total + n2[k]
    count = NX * NY * NZ * NC * PER * WIDTH
    out_ref[...] = out_ref[...] * lax.rsqrt(total / count + EPS)[0:1, 0:1]
    drain()


def on_device(gen, real):
    dma = pltpu.SemaphoreType.DMA
    return pl.pallas_call(
        kernel,
        out_shape=jax.ShapeDtypeStruct((PER, WIDTH), F32),
        in_specs=[pl.BlockSpec(memory_space=pl.ANY)] * 2,
        out_specs=pl.BlockSpec(memory_space=pltpu.VMEM),
        scratch_shapes=[
            pltpu.VMEM((16, PER, WIDTH), BF16),
            pltpu.VMEM((NZ, NC, 2, PER, WIDTH), BF16),
            pltpu.VMEM((ROWS, COLS), F32),
            pltpu.VMEM((ROWS, CHUNK), F32),
            pltpu.VMEM((ROWS, 1), F32),
            pltpu.VMEM((NZ, CHUNK), F32),
            pltpu.VMEM((NZ, CHUNK), F32),
            pltpu.VMEM((16, NZ, CHUNK), F32),
            pltpu.VMEM((16, 4, 128), F32),
            pltpu.VMEM((17, 8, 128), F32),
            pltpu.VMEM((16, 1, 128), F32),
            pltpu.VMEM((16, 1, 128), F32),
            pltpu.VMEM((3, 128, COLS), BF16),
            pltpu.VMEM((SLICES, 3, 4, PER, PIECE), BF16),
            pltpu.VMEM((SLICES, 4, PER, PIECE), F32),
            pltpu.VMEM((SLICES, 4, PER, PIECE), F32),
            pltpu.VMEM((SLICES, 2, 2, PER, PIECE), BF16),
            pltpu.VMEM((SLICES, 2, 4, PER, PIECE), BF16),
            pltpu.VMEM((SLICES, 3, PER, PIECE), BF16),
            pltpu.VMEM((SLICES, 3, PER, PIECE), BF16),
            dma, dma((5,)), dma((SEMS,)), dma((5,)), dma((5,)),
        ],
        compiler_params=pltpu.CompilerParams(
            collective_id=0, has_side_effects=True, vmem_limit_bytes=60 * 1024 * 1024
        ),
    )(gen, real)


def solution(mesh):
    torus = Mesh(mesh.devices.reshape(NZ, NY, NC, NX), AXES)
    return jax.shard_map(
        on_device,
        mesh=torus,
        in_specs=(P(AXES, None), P(AXES, None)),
        out_specs=P(AXES, None),
        check_vma=False,
    )
```
